16 devices in a mesh: dp: 16 (over z, y, x, core).
Axes of the slice: x: 2, y: 2, z: 2, core: 2. Of those that a mesh axis runs over, the one named last changes fastest.
Arguments:
- x_embed: bfloat16 [4096, 512], P('dp')
- positions: int32 [4096], P('dp')
- k_cache: bfloat16 [2, 4096, 32, 8, 64], P(None, 'dp')
- v_cache: bfloat16 [2, 4096, 32, 8, 64], P(None, 'dp')
- ln1_gain: bfloat16 [2, 512], P(None, 'dp')
- ln1_bias: bfloat16 [2, 512], P(None, 'dp')
- ln2_gain: bfloat16 [2, 512], P(None, 'dp')
- ln2_bias: bfloat16 [2, 512], P(None, 'dp')
- w_qkv: bfloat16 [2, 512, 1536], P(None, 'dp')
- b_qkv: bfloat16 [2, 1536], P(None, 'dp')
- w_out: bfloat16 [2, 512, 512], P(None, 'dp')
- b_out: bfloat16 [2, 512], P(None, 'dp')
- w_in: bfloat16 [2, 512, 2048], P(None, 'dp')
- b_in: bfloat16 [2, 2048], P(None, 'dp')
- w_down: bfloat16 [2, 2048, 512], P(None, 'dp')
- b_down: bfloat16 [2, 512], P(None, 'dp')
- lnf_gain: bfloat16 [512], P('dp')
- lnf_bias: bfloat16 [512], P('dp')
Outputs:
- output 1: bfloat16 [4096, 512], P('dp')
- output 2: bfloat16 [2, 4096, 32, 8, 64], P(None, 'dp')
- output 3: bfloat16 [2, 4096, 32, 8, 64], P(None, 'dp')
All inputs are finite; a program needn't handle non-finite values.
Results may differ from the reference program's by a relative error of at most 0.0104128.
Values are sent between devices in bfloat16 or wider.
A program may use at most 1 GiB of HBM per device.

```python
import jax
import jax.numpy as jnp
from jax import lax

LAYERS = 2
BATCH = 4096
SMAX = 32
D = 512
HEADS = 8
FF = 2048
HEAD = 64
ROT = 16

LN_EPS = 1e-5
ROPE_BASE = 10000.0


def setup_inputs(seed: int = 0) -> dict:
    root_key = jax.random.key(seed)
    subkeys = jax.random.split(root_key, 20)

    def normal(key_idx, arr_shape, std_dev):
        return jax.random.normal(subkeys[key_idx], arr_shape, jnp.float32) * std_dev

    cache_shape = (LAYERS, BATCH, SMAX, HEADS, HEAD)
    positions = jax.random.randint(subkeys[1], (BATCH,), 0, SMAX, dtype=jnp.int32)
    positions = positions.at[0].set(SMAX - 1)
    v_mean = normal(3, (LAYERS, BATCH, 1, HEADS, HEAD), 1.0)
    return {
        'x_embed': normal(0, (BATCH, D), 1.0).astype(jnp.bfloat16),
        'positions': positions,
        'k_cache': normal(2, cache_shape, 1.0).astype(jnp.bfloat16),
        'v_cache': (v_mean + normal(4, cache_shape, 0.5)).astype(jnp.bfloat16),
        'ln1_gain': (1.0 + normal(5, (LAYERS, D), 0.2)).astype(jnp.bfloat16),
        'ln1_bias': normal(6, (LAYERS, D), 0.2).astype(jnp.bfloat16),
        'ln2_gain': (1.0 + normal(7, (LAYERS, D), 0.2)).astype(jnp.bfloat16),
        'ln2_bias': normal(8, (LAYERS, D), 0.2).astype(jnp.bfloat16),
        'w_qkv': normal(9, (LAYERS, D, 3 * D), D ** -0.5).astype(jnp.bfloat16),
        'b_qkv': normal(10, (LAYERS, 3 * D), 0.3).astype(jnp.bfloat16),
        'w_out': normal(11, (LAYERS, D, D), D ** -0.5).astype(jnp.bfloat16),
        'b_out': normal(12, (LAYERS, D), 0.3).astype(jnp.bfloat16),
        'w_in': normal(13, (LAYERS, D, FF), D ** -0.5).astype(jnp.bfloat16),
        'b_in': normal(14, (LAYERS, FF), 0.3).astype(jnp.bfloat16),
        'w_down': normal(15, (LAYERS, FF, D), FF ** -0.5).astype(jnp.bfloat16),
        'b_down': normal(16, (LAYERS, D), 0.3).astype(jnp.bfloat16),
        'lnf_gain': (1.0 + normal(17, (D,), 0.2)).astype(jnp.bfloat16),
        'lnf_bias': normal(18, (D,), 0.2).astype(jnp.bfloat16),
    }


def layer_norm(values, ln_gain, ln_bias):
    x_f32 = values.astype(jnp.float32)
    row_mean = jnp.mean(x_f32, axis=-1, keepdims=True)
    centered = x_f32 - row_mean
    row_var = jnp.mean(centered * centered, axis=-1, keepdims=True)
    normed = centered * lax.rsqrt(row_var + LN_EPS)
    return (normed * ln_gain.astype(jnp.float32) + ln_bias.astype(jnp.float32)).astype(jnp.bfloat16)


def rotate(values, cos_t, sin_t):
    half_dim = ROT // 2
    rot_part = values[..., :ROT].astype(jnp.float32)
    turned = jnp.concatenate([-rot_part[..., half_dim:], rot_part[..., :half_dim]], axis=-1)
    mixed = rot_part * cos_t + turned * sin_t
    return jnp.concatenate([mixed.astype(jnp.bfloat16), values[..., ROT:]], axis=-1)


def reference(x_embed, positions, k_cache, v_cache, ln1_gain, ln1_bias, ln2_gain, ln2_bias, w_qkv, b_qkv, w_out, b_out, w_in, b_in, w_down, b_down, lnf_gain, lnf_bias):
    inv_freq = 1.0 / (ROPE_BASE ** (jnp.arange(0, ROT, 2).astype(jnp.float32) / ROT))
    angles = positions.astype(jnp.float32)[:, None] * inv_freq[None, :]
    angles = jnp.concatenate([angles, angles], axis=-1)[:, None, :]
    cos_t = jnp.cos(angles)
    sin_t = jnp.sin(angles)
    slot_ids = jnp.arange(SMAX)
    write_mask = (slot_ids[None, :] == positions[:, None])[:, :, None, None]
    keep_mask = (slot_ids[None, :] <= positions[:, None])[:, None, :]

    def one_layer(hidden, params):
        (k_layer, v_layer, g_one, c_one, g_two, c_two, wqkv_l, bqkv_l, wout_l, bout_l, win_l, bin_l, wdown_l, bdown_l) = params
        h_attn = layer_norm(hidden, g_one, c_one)
        h_mlp = layer_norm(hidden, g_two, c_two)
        qkv_proj = (jnp.dot(h_attn, wqkv_l, preferred_element_type=jnp.float32) + bqkv_l.astype(jnp.float32)).astype(jnp.bfloat16)
        qkv_proj = qkv_proj.reshape(BATCH, HEADS, 3, HEAD)
        q_heads = rotate(qkv_proj[:, :, 0], cos_t, sin_t)
        k_heads = rotate(qkv_proj[:, :, 1], cos_t, sin_t)
        v_heads = qkv_proj[:, :, 2]
        k_layer = jnp.where(write_mask, k_heads[:, None], k_layer)
        v_layer = jnp.where(write_mask, v_heads[:, None], v_layer)
        scores = jnp.einsum('bhd,bshd->bhs', q_heads.astype(jnp.float32), k_layer.astype(jnp.float32)) * (HEAD ** -0.5)
        scores = jnp.where(keep_mask, scores, -jnp.inf)
        attn_probs = jax.nn.softmax(scores, axis=-1).astype(jnp.bfloat16)
        context = jnp.einsum('bhs,bshd->bhd', attn_probs.astype(jnp.float32), v_layer.astype(jnp.float32)).astype(jnp.bfloat16).reshape(BATCH, D)
        attn_out = jnp.dot(context, wout_l, preferred_element_type=jnp.float32) + bout_l.astype(jnp.float32)
        mlp_act = jax.nn.gelu(jnp.dot(h_mlp, win_l, preferred_element_type=jnp.float32) + bin_l.astype(jnp.float32), approximate=False).astype(jnp.bfloat16)
        mlp_out = jnp.dot(mlp_act, wdown_l, preferred_element_type=jnp.float32) + bdown_l.astype(jnp.float32)
        hidden = (hidden.astype(jnp.float32) + attn_out + mlp_out).astype(jnp.bfloat16)
        return hidden, (k_layer, v_layer)

    stacked = (k_cache, v_cache, ln1_gain, ln1_bias, ln2_gain, ln2_bias, w_qkv, b_qkv, w_out, b_out, w_in, b_in, w_down, b_down)
    hidden, (k_new, v_new) = lax.scan(one_layer, x_embed, stacked)
    return layer_norm(hidden, lnf_gain, lnf_bias), k_new, v_new
```

```python
import math

import jax
import jax.numpy as jnp
from jax import lax
from jax.experimental import pallas as pl
from jax.experimental.pallas import tpu as pltpu
from jax.sharding import PartitionSpec as P

LN_EPS = 1e-5
ROPE_BASE = 10000.0
F32 = jnp.float32
BF16 = jnp.bfloat16
MESH = pl.DeviceIdType.MESH
GRID = (2,) * 5

ERF_NUM = (-2.72614225801306e-10, 2.77068142495902e-08, -2.10102402082508e-06,
           -5.69250639462346e-05, -7.34990630326855e-04, -2.95459980854025e-03,
           -1.60960333262415e-02)
ERF_DEN = (-1.45660718464996e-05, -2.13374055278905e-04, -1.68282697438203e-03,
           -7.37332916720468e-03, -1.42647390514189e-02)


def horner(coefs, t):
    acc = jnp.full_like(t, coefs[0])
    for coef in coefs[1:]:
        acc = acc * t + coef
    return acc


def gelu(v):
    u = jnp.clip(v * (0.5 ** 0.5), -4.0, 4.0)
    t = u * u
    erf = u * horner(ERF_NUM, t) / horner(ERF_DEN, t)
    return 0.5 * v * (1.0 + erf)


def normalize(v):
    centered = v - jnp.mean(v, axis=-1, keepdims=True)
    var = jnp.mean(centered * centered, axis=-1, keepdims=True)
    return centered * lax.rsqrt(var + LN_EPS)


QO = ((0, (0, 32), (0, 640), 0), (0, (0, 32), (640, 640), 1),
      (0, (0, 32), (1280, 256), 2), (1, (0, 32), (0, 512), 2))
IN = ((2, (0, 32), (0, 640), 0), (2, (0, 32), (640, 640), 1), (2, (0, 32), (1280, 768), 2))
DOWN = ((3, (0, 48), (0, 512), 0), (3, (48, 48), (0, 512), 1), (3, (96, 32), (0, 512), 2))
PIECES = (
    [(m, 0, r, c, o) for m, r, c, o in QO] + [(4, 0, (0, 8), (0, 128), 0)],
    [(m, 0, r, c, o) for m, r, c, o in IN],
    [(m, 0, r, c, o) for m, r, c, o in DOWN],
    [(m, 1, r, c, o) for m, r, c, o in QO],
    [(m, 1, r, c, o) for m, r, c, o in IN],
    [(m, 1, r, c, o) for m, r, c, o in DOWN],
)
ITEMS = [it for piece in PIECES for it in piece]
N_ITEMS = len(ITEMS)


def kernel(x_ref, pos_ref, vec_in, wq_in, wo_in, wi_in, wd_in, kc_in, vc_in,
           out_ref, ko_ref, vo_ref,
           wq, wo, wi, wd, vecs,
           lnp, bqkv, bin_, qs, kn, vn, sc, pr, ctxt, hcur, h2s, act, accr,
           posb, local_sem, cache_sem, send_sem, recv_sem):
    me = lax.axis_index('dp')
    core = me % 2
    px = (me // 2) % 2
    py = (me // 4) % 2
    pz = me // 8
    peer_core = me + 1 - 2 * core
    peers = (me + 2 - 4 * px, me + 4 - 8 * py, me + 8 - 16 * pz)
    mats = (wq, wo, wi, wd, vecs)
    shards = (wq_in, wo_in, wi_in, wd_in, vec_in)

    local = {}
    order = [(m, l) for l in range(2) for m in (0, 1, 4, 2, 3) if m != 4 or l == 0]
    for i, (m, l) in enumerate(order):
        src = shards[m].at[l] if m != 4 else shards[m]
        local[(m, l)] = pltpu.make_async_copy(
            src, mats[m].at[l, pz, py, px, core], local_sem.at[i])
        local[(m, l)].start()

    barrier = pltpu.get_barrier_semaphore()
    for peer in peers + (peer_core,):
        pl.semaphore_signal(barrier, inc=1, device_id=(peer,), device_id_type=MESH)
    pl.semaphore_wait(barrier, 4)

    def view(item, full):
        m, l, (r0, rn), (c0, cn), _ = item
        at = [slice(None) if ax in full else v for ax, v in ((2, pz), (1, py), (0, px))]
        return mats[m].at[(l, *at, core, pl.ds(r0, rn), pl.ds(c0, cn))]

    sends = {}

    def send(i, stage):
        item = ITEMS[i]
        o = item[4]
        axes = [(o + s) % 3 for s in range(3)]
        if stage < 3:
            ref = view(item, axes[:stage])
            peer = peers[axes[stage]]
        else:
            if stage == 3:
                ref = view(item, axes[:2])
            else:
                m, l, (r0, rn), (c0, cn), _ = item
                own = (px, py, pz)[axes[2]]
                at = [slice(None), slice(None), slice(None)]
                at[2 - axes[2]] = 1 - own
                ref = mats[m].at[(l, *at, core, pl.ds(r0, rn), pl.ds(c0, cn))]
            peer = peer_core
        copy = pltpu.make_async_remote_copy(
            src_ref=ref, dst_ref=ref, send_sem=send_sem.at[i, stage],
            recv_sem=recv_sem.at[i, stage], device_id=(peer,), device_id_type=MESH)
        copy.start()
        sends[(i, stage)] = copy

    starts = [0]
    for piece in PIECES:
        starts.append(starts[-1] + len(piece))

    def ids(p):
        return range(starts[p], starts[p + 1])

    waited = set()

    def a(p):
        for i in ids(p):
            key = (ITEMS[i][0], ITEMS[i][1])
            if key not in waited:
                waited.add(key)
                local[key].wait()
        for i in ids(p):
            send(i, 0)

    def b(p):
        for i in ids(p):
            sends[(i, 0)].wait_recv()
            send(i, 1)

    def c(p):
        for i in ids(p):
            sends[(i, 1)].wait_recv()
            send(i, 2)
            send(i, 3)

    def d(p):
        for i in ids(p):
            sends[(i, 2)].wait_recv()
            send(i, 4)

    def e(p):
        for i in ids(p):
            sends[(i, 3)].wait_recv()
            sends[(i, 4)].wait_recv()

    a(0)
    a(1)
    a(2)
    cache = []
    for l in range(2):
        for j, (src, dst) in enumerate(((kc_in, ko_ref), (vc_in, vo_ref))):
            cp = pltpu.make_async_copy(src.at[l], dst.at[l], cache_sem.at[2 * l + j])
            cp.start()
            cache.append(cp)

    pos = pos_ref[...]
    posf = pos.astype(F32)
    posb[...] = jnp.broadcast_to(posf, (16, 256)).astype(BF16)
    row8 = lax.broadcasted_iota(jnp.int32, (8, 256), 0)
    inv_freq = jnp.full((8, 256), 1.0, F32)
    for i in range(1, 8):
        inv_freq = jnp.where(row8 == i, F32(ROPE_BASE ** (-i / 8.0)), inv_freq)
    angle = jnp.broadcast_to(posf, (8, 256)) * inv_freq
    cos_t = jnp.cos(angle)
    sin_t = jnp.sin(angle)
    hcur[...] = x_ref[...]

    b(0)
    b(1)
    c(0)
    a(3)
    b(2)
    d(0)
    c(1)
    e(0)
    a(4)
    b(3)

    vall = vecs[...].reshape(16, 8, 128).astype(F32)
    lane128 = lax.broadcasted_iota(jnp.int32, (128, 512), 0)
    lane512 = lax.broadcasted_iota(jnp.int32, (128, 512), 1)
    spread = jnp.where(lane128 % 32 == lane512 % 32, 1.0, 0.0).astype(BF16)
    dev_row = lax.broadcasted_iota(jnp.int32, (16, 512), 0)
    own = lax.broadcasted_iota(jnp.int32, (16, 512), 1) // 32 == dev_row
    quarter = lax.broadcasted_iota(jnp.int32, (16, 128), 1) // 32
    qa = lax.broadcasted_iota(jnp.int32, (128, 1536), 0)
    qn = lax.broadcasted_iota(jnp.int32, (128, 1536), 1)
    spread_q = jnp.where(qa == qn % 96, 1.0, 0.0).astype(BF16)
    own_q = (lax.broadcasted_iota(jnp.int32, (16, 1536), 1) // 96
             == lax.broadcasted_iota(jnp.int32, (16, 1536), 0))
    for l in range(2):
        for half in range(2):
            share = vall[:, 4 * l + half, :]
            for k in range(4 if half == 0 else 3):
                part = jnp.where(quarter == k, share, 0.0).astype(BF16)
                wide = jnp.dot(part, spread, preferred_element_type=F32)
                lnp[l, 4 * half + k] = jnp.sum(jnp.where(own, wide, 0.0), axis=0, keepdims=True)
        wide = jnp.dot(vall[:, 4 * l + 2, :].astype(BF16), spread_q, preferred_element_type=F32)
        bqkv[l] = jnp.sum(jnp.where(own_q, wide, 0.0), axis=0, keepdims=True)
        share = vall[:, 4 * l + 3, :]
        for n in range(8):
            bin_[l, n] = jnp.concatenate([share[2 * n:2 * n + 1], share[2 * n + 1:2 * n + 2]], axis=1)

    def rope(t):
        r1, r2 = t[0:8], t[8:16]
        rot = jnp.concatenate([r1 * cos_t - r2 * sin_t, r2 * cos_t + r1 * sin_t, t[16:]], axis=0)
        return rot.astype(BF16)

    def qkv_stage(l):
        normed = normalize(hcur[...].astype(F32))
        h1 = (normed * lnp[l, 0] + lnp[l, 1]).astype(BF16)
        h2s[...] = (normed * lnp[l, 2] + lnp[l, 3]).astype(BF16)
        for j in range(4):
            w = wq[l, :, :, :, :, :, pl.ds(384 * j, 384)].reshape(512, 384)
            y = jnp.dot(h1, w, preferred_element_type=F32) + bqkv[l][:, 384 * j:384 * (j + 1)]
            yt = y.astype(BF16).astype(F32).T
            for g in range(2):
                base = 192 * g
                qs[2 * j + g] = rope(yt[base:base + 64]).astype(F32) * 0.125
                kn[2 * j + g] = rope(yt[base + 64:base + 128])
                vn[2 * j + g] = yt[base + 128:base + 192].astype(BF16)

    def insert(ref, l, s, h, new):
        mask = posb[...] == s.astype(BF16)
        page = ref[l, s, h].reshape(4, 16, 256)
        page = jnp.where(mask[None], new, page).reshape(64, 256)
        ref[l, s, h] = page
        return page.astype(F32)

    def heads(l, h0, h1):
        slot = lax.broadcasted_iota(jnp.int32, (32, 256), 0)
        keep = slot <= pos

        def one_head(h, carry):
            knew = kn[h].reshape(4, 16, 256)
            vnew = vn[h].reshape(4, 16, 256)

            def score(s, carry):
                page = insert(ko_ref, l, s, h, knew)
                sc[pl.ds(s, 1), :] = jnp.sum(page * qs[h], axis=0, keepdims=True)
                return carry

            lax.fori_loop(0, 32, score, 0, unroll=8)
            sm = jnp.where(keep, sc[...], -jnp.inf)
            ex = jnp.exp(sm - jnp.max(sm, axis=0, keepdims=True))
            probs = ex / jnp.sum(ex, axis=0, keepdims=True)
            pr[...] = probs.astype(BF16).astype(F32)

            def mix(s, acc):
                page = insert(vo_ref, l, s, h, vnew)
                return acc + page * pr[pl.ds(s, 1), :]

            ctx = lax.fori_loop(0, 32, mix, jnp.zeros((64, 256), F32), unroll=8)
            ctxt[h] = ctx.astype(BF16).astype(F32)
            return carry

        lax.fori_loop(h0, h1, one_head, 0)

    def attn_out(l):
        ctx = ctxt[...].reshape(512, 256).T.astype(BF16)
        w = wo[l].reshape(512, 512)
        accr[...] = jnp.dot(ctx, w, preferred_element_type=F32) + lnp[l, 4]

    def mlp_in(l):
        def chunk(n, carry):
            cols = pl.ds(pl.multiple_of(n * 256, 256), 256)
            w = wi[l, :, :, :, :, :, cols].reshape(512, 256)
            y = jnp.dot(h2s[...], w, preferred_element_type=F32) + bin_[l, n]
            act[:, cols] = gelu(y).astype(BF16)
            return carry

        lax.fori_loop(0, 8, chunk, 0)

    def mlp_down(l):
        for j in range(2):
            cols = slice(256 * j, 256 * (j + 1))
            w = wd[l, :, :, :, :, :, cols].reshape(2048, 256)
            m = jnp.dot(act[...], w, preferred_element_type=F32) + lnp[l, 5][:, cols]
            hcur[:, cols] = (hcur[:, cols].astype(F32) + accr[:, cols] + m).astype(BF16)

    qkv_stage(0)
    c(2)
    cache[0].wait()
    cache[1].wait()
    heads(0, 0, 4)
    d(1)
    heads(0, 4, 8)
    a(5)
    b(4)
    attn_out(0)
    e(1)
    c(3)
    mlp_in(0)
    d(2)
    e(2)
    b(5)
    mlp_down(0)
    d(3)
    c(4)
    e(3)
    qkv_stage(1)
    cache[2].wait()
    cache[3].wait()
    heads(1, 0, 4)
    c(5)
    d(4)
    heads(1, 4, 8)
    attn_out(1)
    e(4)
    mlp_in(1)
    d(5)
    e(5)
    mlp_down(1)
    out_ref[...] = (normalize(hcur[...].astype(F32)) * lnp[0, 6] + lnp[1, 6]).astype(BF16)
    for copy in sends.values():
        copy.wait_send()


def solution(mesh):
    row_spec = P('dp', None)
    vec_spec = P(None, 'dp')
    mat_spec = P(None, 'dp', None)
    cache_spec = P(None, 'dp', None, None, None)
    in_specs = (row_spec, P('dp'), cache_spec, cache_spec, vec_spec, vec_spec, vec_spec, vec_spec, mat_spec, vec_spec, mat_spec, vec_spec, mat_spec, vec_spec, mat_spec, vec_spec, P('dp'), P('dp'))
    out_specs = (row_spec, cache_spec, cache_spec)

    def device_step(x_embed, positions, k_cache, v_cache, ln1_gain, ln1_bias, ln2_gain, ln2_bias, w_qkv, b_qkv, w_out, b_out, w_in, b_in, w_down, b_down, lnf_gain, lnf_bias):
        pad = jnp.zeros((2, 32), BF16)
        lnf = jnp.stack([lnf_gain, lnf_bias])
        vec = jnp.concatenate([ln1_gain, ln1_bias, ln2_gain, ln2_bias, b_out, b_down, lnf, pad, b_qkv, pad, b_in], axis=1)
        vec = vec.reshape(8, 128)
        to_lanes = (0, 2, 3, 4, 1)
        kt = jnp.transpose(k_cache, to_lanes)
        vt = jnp.transpose(v_cache, to_lanes)
        vmem = pl.BlockSpec(memory_space=pltpu.VMEM)
        hbm = pl.BlockSpec(memory_space=pl.ANY)
        cache_shape = (2, 32, 8, 64, 256)
        out, ko, vo = pl.pallas_call(
            kernel,
            out_shape=(jax.ShapeDtypeStruct((256, 512), BF16),
                       pltpu.VMEM(cache_shape, BF16), pltpu.VMEM(cache_shape, BF16)),
            in_specs=[vmem, vmem, hbm, hbm, hbm, hbm, hbm, hbm, hbm],
            out_specs=(vmem, vmem, vmem),
            scratch_shapes=[
                pltpu.VMEM(GRID + (32, 1536), BF16),
                pltpu.VMEM(GRID + (32, 512), BF16),
                pltpu.VMEM(GRID + (32, 2048), BF16),
                pltpu.VMEM(GRID + (128, 512), BF16),
                pltpu.VMEM((1,) + GRID[1:] + (8, 128), BF16),
                pltpu.VMEM((2, 8, 1, 512), F32),
                pltpu.VMEM((2, 1, 1536), F32),
                pltpu.VMEM((2, 8, 1, 256), F32),
                pltpu.VMEM((8, 64, 256), F32),
                pltpu.VMEM((8, 64, 256), BF16),
                pltpu.VMEM((8, 64, 256), BF16),
                pltpu.VMEM((32, 256), F32),
                pltpu.VMEM((32, 256), F32),
                pltpu.VMEM((8, 64, 256), F32),
                pltpu.VMEM((256, 512), BF16),
                pltpu.VMEM((256, 512), BF16),
                pltpu.VMEM((256, 2048), BF16),
                pltpu.VMEM((256, 512), F32),
                pltpu.VMEM((16, 256), BF16),
                pltpu.SemaphoreType.DMA((9,)),
                pltpu.SemaphoreType.DMA((4,)),
                pltpu.SemaphoreType.DMA((N_ITEMS, 5)),
                pltpu.SemaphoreType.DMA((N_ITEMS, 5)),
            ],
            compiler_params=pltpu.CompilerParams(
                collective_id=0, has_side_effects=True, vmem_limit_bytes=26 * 2 ** 20),
        )(x_embed, positions.reshape(1, 256), vec, w_qkv, w_out, w_in, w_down, kt, vt)
        back = (0, 4, 1, 2, 3)
        return out, jnp.transpose(ko, back), jnp.transpose(vo, back)

    return jax.shard_map(device_step, mesh=mesh, in_specs=in_specs, out_specs=out_specs, check_vma=False)
```

```python
import jax
import jax.numpy as jnp
from jax import lax
from jax.experimental import pallas as pl
from jax.experimental.pallas import tpu as pltpu
from jax.sharding import PartitionSpec as P

LN_EPS = 1e-5
ROPE_BASE = 10000.0
F32 = jnp.float32
BF16 = jnp.bfloat16
MESH = pl.DeviceIdType.MESH
GRID = (2,) * 5
LAYERS, SEQS, WIDTH, SLOTS, HEADS, HEAD, LANES, FF = 2, 256, 512, 32, 8, 64, 128, 2048
PAIR = 6 * HEAD
EARLY = 2
ALL = slice(None)
SCOPED = 22 * 2 ** 20

ERF_NUM = (-2.72614225801306e-10, 2.77068142495902e-08, -2.10102402082508e-06,
           -5.69250639462346e-05, -7.34990630326855e-04, -2.95459980854025e-03,
           -1.60960333262415e-02)
ERF_DEN = (-1.45660718464996e-05, -2.13374055278905e-04, -1.68282697438203e-03,
           -7.37332916720468e-03, -1.42647390514189e-02)


def horner(coefs, t):
    acc = jnp.full_like(t, coefs[0])
    for coef in coefs[1:]:
        acc = acc * t + coef
    return acc


def gelu(v):
    u = jnp.clip(v * (0.5 ** 0.5), -4.0, 4.0)
    t = u * u
    erf = u * horner(ERF_NUM, t) / horner(ERF_DEN, t)
    return 0.5 * v * (1.0 + erf)


def normalize(v):
    centered = v - jnp.mean(v, axis=-1, keepdims=True)
    var = jnp.mean(centered * centered, axis=-1, keepdims=True)
    return centered * lax.rsqrt(var + LN_EPS)


def dot(a, b):
    return jnp.dot(a, b, preferred_element_type=F32)


def iota(shape, axis):
    return lax.broadcasted_iota(jnp.int32, shape, axis)


def pieces(l):
    rows = (l, 0, SLOTS)
    third = 5 * LANES
    qo = [(0, *rows, 0, third, 0), (0, *rows, third, third, 1),
          (0, *rows, 2 * third, 2 * LANES, 2), (1, *rows, 0, WIDTH, 2)]
    up = [(2, *rows, 0, third, 0), (2, *rows, third, third, 1), (2, *rows, 2 * third, 6 * LANES, 2)]
    down = [(3, l, 0, 48, 0, WIDTH, 0), (3, l, 48, 48, 0, WIDTH, 1), (3, l, 96, SLOTS, 0, WIDTH, 2)]
    return [qo, up, down]


PIECES = pieces(0) + pieces(1) + [[(4, 0, 0, HEADS, 0, LANES, 0)]]
VEC = len(PIECES) - 1
N_VEC = 10
ITEMS = [item for piece in PIECES for item in piece]
FIRST = [sum(len(piece) for piece in PIECES[:p]) for p in range(len(PIECES) + 1)]


def attend(h, pos, posb, qs, kn, vn, k_in, v_in, k_out, v_out, sc, pr, ctxt):
    tiles = (HEAD // 16, 16, SEQS)
    knew = kn[h].reshape(tiles)
    vnew = vn[h].reshape(tiles)

    def insert(src, dst, s, new):
        mask = posb[...] == s.astype(BF16)
        page = jnp.where(mask[None], new, src(s).reshape(tiles)).reshape(HEAD, SEQS)
        dst(s, page)
        return page.astype(F32)

    def score(s, carry):
        page = insert(k_in, k_out, s, knew)
        sc[pl.ds(s, 1), :] = jnp.sum(page * qs[h], axis=0, keepdims=True)
        return carry

    lax.fori_loop(0, SLOTS, score, 0, unroll=8)
    sm = jnp.where(iota((SLOTS, SEQS), 0) <= pos, sc[...], -jnp.inf)
    ex = jnp.exp(sm - jnp.max(sm, axis=0, keepdims=True))
    probs = ex / jnp.sum(ex, axis=0, keepdims=True)
    pr[...] = probs.astype(BF16).astype(F32)

    def mix(s, acc):
        page = insert(v_in, v_out, s, vnew)
        return acc + page * pr[pl.ds(s, 1), :]

    ctx = lax.fori_loop(0, SLOTS, mix, jnp.zeros((HEAD, SEQS), F32), unroll=8)
    ctxt[h] = ctx.astype(BF16).astype(F32)


def attn_out(ctxt, w, bias):
    ctx = ctxt[...].reshape(WIDTH, SEQS).T.astype(BF16)
    return dot(ctx, w.reshape(WIDTH, WIDTH)) + bias


def gather_kernel(x_ref, pos_ref, *refs):
    gather_body(x_ref, pos_ref, refs[:N_VEC], *refs[N_VEC:])


def gather_body(x_ref, pos_ref, vec_in, wq_in, wo_in, wi_in, wd_in, kc_in, vc_in,
                  ko0, vo0, ko1, vo1, wo1, wd1, qs, kn, vn, ctxt, hcur, act, lnp,
                  wq, wo0, wi, wd0, vecs, bqkv, bin_, sc, pr, h2s, accr, posb,
                  local_sem, cache_sem, send_sem, recv_sem):
    me = lax.axis_index('dp')
    core = me % 2
    px = (me // 2) % 2
    py = (me // 4) % 2
    pz = me // 8
    place = (px, py, pz)
    peer_core = me + 1 - 2 * core
    peers = (me + 2 - 4 * px, me + 4 - 8 * py, me + 8 - 16 * pz)
    shards = (wq_in, wo_in, wi_in, wd_in)

    def whole(m, l):
        if m == 4:
            return vecs
        return ((wq.at[0], wo0, wi.at[0], wd0), (wq.at[1], wo1, wi.at[1], wd1))[l][m]

    local = {}
    for l, m in [(l, m) for l in range(LAYERS) for m in range(4)]:
        local[(m, l)] = pltpu.make_async_copy(
            shards[m].at[l], whole(m, l).at[pz, py, px, core], local_sem.at[len(local)])
        local[(m, l)].start()

    barrier = pltpu.get_barrier_semaphore()
    for peer in peers + (peer_core,):
        pl.semaphore_signal(barrier, inc=1, device_id=(peer,), device_id_type=MESH)
    g1, b1, g2, b2, bo, bd, bq, bi, gf, bf = (ref[...].astype(F32) for ref in vec_in)
    pad = jnp.zeros((LAYERS, 32), F32)
    groups = ([g1, b1, g2, b2], [bo, bd, jnp.concatenate([gf, bf], axis=0), pad], [bq, pad])
    rows = [jnp.concatenate(group, axis=1) for group in groups] + [bi]
    vecs[pz, py, px, core] = jnp.concatenate(rows, axis=0).astype(BF16)
    pl.semaphore_wait(barrier, len(peers) + 1)

    sends = {}

    def send(i, stage):
        m, l, r0, rn, c0, cn, o = ITEMS[i]
        axes = [(o + s) % 3 for s in range(3)]
        at = [place[2], place[1], place[0]]
        for ax in axes[:min(stage, 2)]:
            at[2 - ax] = ALL
        if stage == 4:
            at[2 - axes[2]] = 1 - place[axes[2]]
        ref = whole(m, l).at[(*at, core, pl.ds(r0, rn), pl.ds(c0, cn))]
        peer = peers[axes[stage]] if stage < 3 else peer_core
        copy = pltpu.make_async_remote_copy(
            src_ref=ref, dst_ref=ref, send_sem=send_sem.at[i, stage],
            recv_sem=recv_sem.at[i, stage], device_id=(peer,), device_id_type=MESH)
        copy.start()
        sends[(i, stage)] = copy

    def ids(p):
        return range(FIRST[p], FIRST[p + 1])

    waited = set()

    def a(p):
        for i in ids(p):
            key = ITEMS[i][:2]
            if key in local and key not in waited:
                waited.add(key)
                local[key].wait()
        for i in ids(p):
            send(i, 0)

    def b(p):
        for i in ids(p):
            sends[(i, 0)].wait_recv()
            send(i, 1)

    def c(p):
        for i in ids(p):
            sends[(i, 1)].wait_recv()
            send(i, 2)
            send(i, 3)

    def d(p):
        for i in ids(p):
            sends[(i, 2)].wait_recv()
            send(i, 4)

    def e(p):
        for i in ids(p):
            sends[(i, 3)].wait_recv()
            sends[(i, 4)].wait_recv()

    a(0)
    a(VEC)
    a(1)
    a(2)
    cache = []
    ko, vo = (ko0, ko1), (vo0, vo1)
    for l in range(LAYERS):
        for src, dst in ((kc_in, ko), (vc_in, vo)):
            cache.append(pltpu.make_async_copy(src.at[l], dst[l], cache_sem.at[len(cache)]))
            cache[-1].start()

    pos = pos_ref[...]
    posf = pos.astype(F32)
    posb[...] = jnp.broadcast_to(posf, posb.shape).astype(BF16)
    half = (8, SEQS)
    inv_freq = jnp.full(half, 1.0, F32)
    for i in range(1, 8):
        inv_freq = jnp.where(iota(half, 0) == i, F32(ROPE_BASE ** (-i / 8.0)), inv_freq)
    angle = jnp.broadcast_to(posf, half) * inv_freq
    cos_t = jnp.cos(angle)
    sin_t = jnp.sin(angle)
    hcur[...] = x_ref[...]

    b(VEC)
    b(0)
    b(1)
    c(VEC)
    c(0)
    a(3)
    b(2)
    d(VEC)
    e(VEC)

    vall = vecs[...].reshape(16, 8, LANES).astype(F32)
    wide_shape = (16, WIDTH)
    spread = jnp.where(iota((LANES, WIDTH), 0) % 32 == iota((LANES, WIDTH), 1) % 32, 1.0, 0.0).astype(BF16)
    own = iota(wide_shape, 1) // 32 == iota(wide_shape, 0)
    quarter = iota((16, LANES), 1) // 32
    qkv_shape = (LANES, 3 * WIDTH)
    spread_q = jnp.where(iota(qkv_shape, 0) == iota(qkv_shape, 1) % 96, 1.0, 0.0).astype(BF16)
    own_q = iota((16, 3 * WIDTH), 1) // 96 == iota((16, 3 * WIDTH), 0)

    def collapse(mask, part, table):
        return jnp.sum(jnp.where(mask, dot(part.astype(BF16), table), 0.0), axis=0, keepdims=True)

    for l in range(LAYERS):
        for k in range(7):
            part = jnp.where(quarter == k % 4, vall[:, 2 * (k // 4) + l, :], 0.0)
            lnp[l, k] = collapse(own, part, spread)
        bqkv[l] = collapse(own_q, vall[:, 4 + l, :], spread_q)
        share = vall[:, 6 + l, :]
        for n in range(8):
            bin_[l, n] = jnp.concatenate([share[2 * n:2 * n + 1], share[2 * n + 1:2 * n + 2]], axis=1)

    def rope(t):
        r1, r2 = t[:8], t[8:16]
        rot = jnp.concatenate([r1 * cos_t - r2 * sin_t, r2 * cos_t + r1 * sin_t, t[16:]], axis=0)
        return rot.astype(BF16)

    def qkv_stage(l):
        normed = normalize(hcur[...].astype(F32))
        h1 = (normed * lnp[l, 0] + lnp[l, 1]).astype(BF16)
        h2s[...] = (normed * lnp[l, 2] + lnp[l, 3]).astype(BF16)
        for j in range(HEADS // 2):
            cols = slice(PAIR * j, PAIR * (j + 1))
            y = dot(h1, whole(0, l)[:, :, :, :, :, cols].reshape(WIDTH, PAIR)) + bqkv[l][:, cols]
            yt = y.astype(BF16).astype(F32).T
            for g in range(2):
                q, k, v = (yt[HEAD * (3 * g + i):HEAD * (3 * g + i + 1)] for i in range(3))
                qs[2 * j + g] = rope(q).astype(F32) * (HEAD ** -0.5)
                kn[2 * j + g] = rope(k)
                vn[2 * j + g] = v.astype(BF16)

    def heads(l, h0, h1):
        def one_head(h, carry):
            def put(ref):
                def store(s, page):
                    ref[s, h] = page
                return store
            attend(h, pos, posb, qs, kn, vn, lambda s: ko[l][s, h], lambda s: vo[l][s, h],
                   put(ko[l]), put(vo[l]), sc, pr, ctxt)
            return carry

        lax.fori_loop(h0, h1, one_head, 0)

    def mlp_in(l, n0, n1):
        def chunk(n, carry):
            cols = pl.ds(pl.multiple_of(n * SEQS, SEQS), SEQS)
            w = whole(2, l)[:, :, :, :, :, cols].reshape(WIDTH, SEQS)
            y = dot(h2s[...], w) + bin_[l, n]
            act[:, cols] = gelu(y).astype(BF16)
            return carry

        lax.fori_loop(n0, n1, chunk, 0)

    c(1)
    d(0)
    a(4)
    b(3)
    e(0)
    c(2)
    qkv_stage(0)
    cache[0].wait()
    cache[1].wait()
    heads(0, 0, 4)
    a(5)
    b(4)
    d(1)
    heads(0, 4, 6)
    c(3)
    heads(0, 6, HEADS)
    accr[...] = attn_out(ctxt, wo0[...], lnp[0, 4])
    e(1)
    b(5)
    mlp_in(0, 0, 4)
    d(2)
    mlp_in(0, 4, 8)
    c(4)
    e(2)
    for j in range(2):
        cols = slice(SEQS * j, SEQS * (j + 1))
        m = dot(act[...], wd0[:, :, :, :, :, cols].reshape(FF, SEQS)) + lnp[0, 5][:, cols]
        hcur[:, cols] = (hcur[:, cols].astype(F32) + accr[:, cols] + m).astype(BF16)
    d(3)
    c(5)
    e(3)
    qkv_stage(1)
    cache[2].wait()
    cache[3].wait()
    heads(1, 0, EARLY)
    d(4)
    e(4)
    mlp_in(1, 0, 4)
    d(5)
    mlp_in(1, 4, 8)
    e(5)
    for copy in sends.values():
        copy.wait_send()


def finish_kernel(ko0, vo0, ko1, vo1, wo1, wd1, qs, kn, vn, ctxt, hcur, act, lnp, pos_ref,
                  out_ref, k_hbm, v_hbm, kst, vst, ctxs, sc, pr, posb, sems):
    last = LAYERS - 1
    copies = []

    def write(src, dst):
        copies.append(pltpu.make_async_copy(src, dst, sems.at[len(copies)]))
        copies[-1].start()

    for src, dst in ((ko0, k_hbm), (vo0, v_hbm)):
        for g in range(2):
            part = pl.ds(g * (SLOTS // 2), SLOTS // 2)
            write(src.at[part], dst.at[0, part])
    for src, dst in ((ko1, k_hbm), (vo1, v_hbm)):
        write(src.at[:, pl.ds(0, EARLY)], dst.at[last, :, pl.ds(0, EARLY)])
    pos = pos_ref[...]
    posb[...] = jnp.broadcast_to(pos.astype(F32), posb.shape).astype(BF16)
    ctxs[...] = ctxt[...]

    def put(ref, i):
        def store(s, page):
            ref[i, s] = page
        return store

    for i in range(HEADS - EARLY):
        h = EARLY + i
        attend(h, pos, posb, qs, kn, vn, lambda s: ko1[s, h], lambda s: vo1[s, h],
               put(kst, i), put(vst, i), sc, pr, ctxs)
        write(kst.at[i], k_hbm.at[last, :, h])
        write(vst.at[i], v_hbm.at[last, :, h])
    x = attn_out(ctxs, wo1[...], lnp[last, 4])
    m = dot(act[...], wd1[...].reshape(FF, WIDTH)) + lnp[last, 5]
    x = (hcur[...].astype(F32) + x + m).astype(BF16).astype(F32)
    out_ref[...] = (normalize(x) * lnp[0, 6] + lnp[1, 6]).astype(BF16)
    for copy in copies:
        copy.wait()


def solution(mesh):
    row_spec = P('dp', None)
    vec_spec = P(None, 'dp')
    mat_spec = P(None, 'dp', None)
    cache_spec = P(None, 'dp', None, None, None)
    in_specs = (row_spec, P('dp'), cache_spec, cache_spec, vec_spec, vec_spec, vec_spec, vec_spec, mat_spec, vec_spec, mat_spec, vec_spec, mat_spec, vec_spec, mat_spec, vec_spec, P('dp'), P('dp'))
    out_specs = (row_spec, cache_spec, cache_spec)

    def device_step(x_embed, positions, k_cache, v_cache, ln1_gain, ln1_bias, ln2_gain, ln2_bias, w_qkv, b_qkv, w_out, b_out, w_in, b_in, w_down, b_down, lnf_gain, lnf_bias):
        vectors = (ln1_gain, ln1_bias, ln2_gain, ln2_bias, b_out, b_down, b_qkv, b_in,
                   lnf_gain.reshape(1, 32), lnf_bias.reshape(1, 32))
        to_lanes = (0, 2, 3, 4, 1)
        kt = jnp.transpose(k_cache, to_lanes)
        vt = jnp.transpose(v_cache, to_lanes)
        pos = positions.reshape(1, SEQS)
        vmem = pl.BlockSpec(memory_space=pltpu.VMEM)
        hbm = pl.BlockSpec(memory_space=pl.ANY)
        cache_shape = (LAYERS, SLOTS, HEADS, HEAD, SEQS)
        head_shape = (HEADS, HEAD, SEQS)
        out_w = GRID[1:] + (SLOTS, WIDTH)
        down_w = GRID[1:] + (LANES, WIDTH)
        carried = [pltpu.VMEM(shape, dtype) for shape, dtype in (
            *[(cache_shape[1:], BF16)] * 4, (out_w, BF16), (down_w, BF16),
            (head_shape, F32), (head_shape, BF16), (head_shape, BF16), (head_shape, F32),
            ((SEQS, WIDTH), BF16), ((SEQS, FF), BF16), ((LAYERS, 8, 1, WIDTH), F32))]
        state = pl.pallas_call(
            gather_kernel,
            out_shape=carried,
            in_specs=[vmem] * (2 + N_VEC) + [hbm] * 6,
            out_specs=[vmem] * len(carried),
            scratch_shapes=[
                pltpu.VMEM(GRID + (SLOTS, 3 * WIDTH), BF16),
                pltpu.VMEM(out_w, BF16),
                pltpu.VMEM(GRID + (SLOTS, FF), BF16),
                pltpu.VMEM(down_w, BF16),
                pltpu.VMEM(GRID[1:] + (8, LANES), BF16),
                pltpu.VMEM((LAYERS, 1, 3 * WIDTH), F32),
                pltpu.VMEM((LAYERS, 8, 1, SEQS), F32),
                pltpu.VMEM((SLOTS, SEQS), F32),
                pltpu.VMEM((SLOTS, SEQS), F32),
                pltpu.VMEM((SEQS, WIDTH), BF16),
                pltpu.VMEM((SEQS, WIDTH), F32),
                pltpu.VMEM((16, SEQS), BF16),
                pltpu.SemaphoreType.DMA((8,)),
                pltpu.SemaphoreType.DMA((4,)),
                pltpu.SemaphoreType.DMA((len(ITEMS), 5)),
                pltpu.SemaphoreType.DMA((len(ITEMS), 5)),
            ],
            compiler_params=pltpu.CompilerParams(
                collective_id=0, has_side_effects=True, vmem_limit_bytes=SCOPED),
        )(x_embed, pos, *vectors, w_qkv, w_out, w_in, w_down, kt, vt)
        state = [pltpu.with_memory_space_constraint(array, pltpu.VMEM) for array in state]
        stage = pltpu.VMEM((HEADS - EARLY, SLOTS, HEAD, SEQS), BF16)
        out, ko, vo = pl.pallas_call(
            finish_kernel,
            out_shape=(jax.ShapeDtypeStruct((SEQS, WIDTH), BF16),
                       pltpu.HBM(cache_shape, BF16), pltpu.HBM(cache_shape, BF16)),
            in_specs=[vmem] * (len(carried) + 1),
            out_specs=(vmem, pl.BlockSpec(memory_space=pltpu.HBM), pl.BlockSpec(memory_space=pltpu.HBM)),
            scratch_shapes=[
                stage, stage,
                pltpu.VMEM(head_shape, F32),
                pltpu.VMEM((SLOTS, SEQS), F32),
                pltpu.VMEM((SLOTS, SEQS), F32),
                pltpu.VMEM((16, SEQS), BF16),
                pltpu.SemaphoreType.DMA((6 + 2 * (HEADS - EARLY),)),
            ],
            compiler_params=pltpu.CompilerParams(vmem_limit_bytes=SCOPED),
        )(*state, pos)
        back = (0, 4, 1, 2, 3)
        return out, jnp.transpose(ko, back), jnp.transpose(vo, back)

    return jax.shard_map(device_step, mesh=mesh, in_specs=in_specs, out_specs=out_specs, check_vma=False)
```

```python
import jax
import jax.numpy as jnp
from jax import lax
from jax.experimental import pallas as pl
from jax.experimental.pallas import tpu as pltpu
from jax.sharding import PartitionSpec as P

LN_EPS = 1e-5
ROPE_BASE = 10000.0
F32 = jnp.float32
BF16 = jnp.bfloat16
MESH = pl.DeviceIdType.MESH
GRID = (2,) * 5
LAYERS, SEQS, WIDTH, SLOTS, HEADS, HEAD, LANES, FF = 2, 256, 512, 32, 8, 64, 128, 2048
PAIR = 6 * HEAD
EARLY = 2
ALL = slice(None)
SCOPED = 20 * 2 ** 20

ERF_NUM = (-2.72614225801306e-10, 2.77068142495902e-08, -2.10102402082508e-06,
           -5.69250639462346e-05, -7.34990630326855e-04, -2.95459980854025e-03,
           -1.60960333262415e-02)
ERF_DEN = (-1.45660718464996e-05, -2.13374055278905e-04, -1.68282697438203e-03,
           -7.37332916720468e-03, -1.42647390514189e-02)


def horner(coefs, t):
    acc = jnp.full_like(t, coefs[0])
    for coef in coefs[1:]:
        acc = acc * t + coef
    return acc


def gelu(v):
    u = jnp.clip(v * (0.5 ** 0.5), -4.0, 4.0)
    t = u * u
    erf = u * horner(ERF_NUM, t) / horner(ERF_DEN, t)
    return 0.5 * v * (1.0 + erf)


def normalize(v):
    centered = v - jnp.mean(v, axis=-1, keepdims=True)
    var = jnp.mean(centered * centered, axis=-1, keepdims=True)
    return centered * lax.rsqrt(var + LN_EPS)


def dot(a, b):
    return jnp.dot(a, b, preferred_element_type=F32)


def iota(shape, axis):
    return lax.broadcasted_iota(jnp.int32, shape, axis)


def pieces(l):
    rows = (l, 0, SLOTS)
    third = 5 * LANES
    qo = [(0, *rows, 0, third, 0), (0, *rows, third, third, 1),
          (0, *rows, 2 * third, 2 * LANES, 2), (1, *rows, 0, WIDTH, 2)]
    up = [(2, *rows, 0, third, 0), (2, *rows, third, third, 1), (2, *rows, 2 * third, 6 * LANES, 2)]
    down = [(3, l, 0, 48, 0, WIDTH, 0), (3, l, 48, 48, 0, WIDTH, 1), (3, l, 96, SLOTS, 0, WIDTH, 2)]
    return [qo, up, down]


PIECES = pieces(0) + pieces(1) + [[(4, 0, 0, HEADS, 0, LANES, 0)]]
VEC = len(PIECES) - 1
N_VEC = 10
ITEMS = [item for piece in PIECES for item in piece]
FIRST = [sum(len(piece) for piece in PIECES[:p]) for p in range(len(PIECES) + 1)]


def attend(h, pos, posb, qs, kn, vn, k_in, v_in, k_out, v_out, sc, pr, ctxt):
    tiles = (HEAD // 16, 16, SEQS)
    knew = kn[h].reshape(tiles)
    vnew = vn[h].reshape(tiles)

    def insert(src, dst, s, new):
        mask = posb[...] == s.astype(BF16)
        page = jnp.where(mask[None], new, src(s).reshape(tiles)).reshape(HEAD, SEQS)
        dst(s, page)
        return page.astype(F32)

    def score(s, carry):
        page = insert(k_in, k_out, s, knew)
        sc[pl.ds(s, 1), :] = jnp.sum(page * qs[h], axis=0, keepdims=True)
        return carry

    lax.fori_loop(0, SLOTS, score, 0, unroll=8)
    sm = jnp.where(iota((SLOTS, SEQS), 0) <= pos, sc[...], -jnp.inf)
    ex = jnp.exp(sm - jnp.max(sm, axis=0, keepdims=True))
    probs = ex / jnp.sum(ex, axis=0, keepdims=True)
    pr[...] = probs.astype(BF16).astype(F32)

    def mix(s, acc):
        page = insert(v_in, v_out, s, vnew)
        return acc + page * pr[pl.ds(s, 1), :]

    ctx = lax.fori_loop(0, SLOTS, mix, jnp.zeros((HEAD, SEQS), F32), unroll=8)
    ctxt[h] = ctx.astype(BF16).astype(F32)


def attn_out(ctxt, w, bias):
    ctx = ctxt[...].reshape(WIDTH, SEQS).T.astype(BF16)
    return dot(ctx, w.reshape(WIDTH, WIDTH)) + bias


def mlp_in(h, w_ref, bias_ref, l, act, n0, n1):
    for n in range(n0, n1):
        cols = slice(n * SEQS, (n + 1) * SEQS)
        w = w_ref[:, :, :, :, :, cols].reshape(WIDTH, SEQS)
        act[:, cols] = gelu(dot(h[...], w) + bias_ref[l, n]).astype(BF16)


def gather_kernel(x_in, pos_in, *refs):
    gather_body(x_in, pos_in, refs[:N_VEC], *refs[N_VEC:-N_VEC], refs[-N_VEC:])


def gather_body(x_in, pos_in, vec_in, wq_in, wo_in, wi_in, wd_in, kc_in, vc_in,
                  ko0, vo0, ko1, vo1, wo1, wi1, wd1, qs, kn, vn, ctxt, hcur, h2s, lnp, bin_, pos_ref,
                  wq, wo0, wi0, wd0, vecs, bqkv, sc, pr, act, accr, posb,
                  local_sem, cache_sem, small_sem, send_sem, recv_sem, vec_ref):
    me = lax.axis_index('dp')
    core = me % 2
    px = (me // 2) % 2
    py = (me // 4) % 2
    pz = me // 8
    place = (px, py, pz)
    peer_core = me + 1 - 2 * core
    peers = (me + 2 - 4 * px, me + 4 - 8 * py, me + 8 - 16 * pz)
    shards = (wq_in, wo_in, wi_in, wd_in)

    def whole(m, l):
        if m == 4:
            return vecs
        return ((wq.at[0], wo0, wi0, wd0), (wq.at[1], wo1, wi1, wd1))[l][m]

    local = {}
    for l, m in [(l, m) for l in range(LAYERS) for m in range(4)]:
        local[(m, l)] = pltpu.make_async_copy(
            shards[m].at[l], whole(m, l).at[pz, py, px, core], local_sem.at[len(local)])
    for m in range(2):
        local[(m, 0)].start()
    barrier = pltpu.get_barrier_semaphore()
    for peer in peers + (peer_core,):
        pl.semaphore_signal(barrier, inc=1, device_id=(peer,), device_id_type=MESH)
    small = []
    for src, dst in zip((*vec_in, pos_in, x_in), (*vec_ref, pos_ref, hcur)):
        small.append(pltpu.make_async_copy(src, dst, small_sem.at[len(small)]))
        small[-1].start()
    for key, copy in local.items():
        if key not in ((0, 0), (1, 0)):
            copy.start()
    pl.semaphore_wait(barrier, len(peers) + 1)

    sends = {}

    def send(i, stage):
        m, l, r0, rn, c0, cn, o = ITEMS[i]
        axes = [(o + s) % 3 for s in range(3)]
        at = [place[2], place[1], place[0]]
        for ax in axes[:min(stage, 2)]:
            at[2 - ax] = ALL
        if stage == 4:
            at[2 - axes[2]] = 1 - place[axes[2]]
        ref = whole(m, l).at[(*at, core, pl.ds(r0, rn), pl.ds(c0, cn))]
        peer = peers[axes[stage]] if stage < 3 else peer_core
        copy = pltpu.make_async_remote_copy(
            src_ref=ref, dst_ref=ref, send_sem=send_sem.at[i, stage],
            recv_sem=recv_sem.at[i, stage], device_id=(peer,), device_id_type=MESH)
        copy.start()
        sends[(i, stage)] = copy

    def ids(p):
        return range(FIRST[p], FIRST[p + 1])

    waited = set()

    def a(p):
        for i in ids(p):
            key = ITEMS[i][:2]
            if key in local and key not in waited:
                waited.add(key)
                local[key].wait()
        for i in ids(p):
            send(i, 0)

    def b(p):
        for i in ids(p):
            sends[(i, 0)].wait_recv()
            send(i, 1)

    def c(p):
        for i in ids(p):
            sends[(i, 1)].wait_recv()
            send(i, 2)
            send(i, 3)

    def d(p):
        for i in ids(p):
            sends[(i, 2)].wait_recv()
            send(i, 4)

    def e(p):
        for i in ids(p):
            sends[(i, 3)].wait_recv()
            sends[(i, 4)].wait_recv()

    a(0)
    for copy in small[:N_VEC]:
        copy.wait()
    g1, b1, g2, b2, bo, bd, bq, bi, gf, bf = (ref[...].astype(F32) for ref in vec_ref)
    pad = jnp.zeros((LAYERS, 32), F32)
    groups = ([g1, b1, g2, b2], [bo, bd, jnp.concatenate([gf, bf], axis=0), pad], [bq, pad])
    rows = [jnp.concatenate(group, axis=1) for group in groups] + [bi]
    vecs[pz, py, px, core] = jnp.concatenate(rows, axis=0).astype(BF16)
    a(VEC)
    a(1)
    a(2)
    cache = []
    ko, vo = (ko0, ko1), (vo0, vo1)
    for l in range(LAYERS):
        for src, dst in ((kc_in, ko), (vc_in, vo)):
            cache.append(pltpu.make_async_copy(src.at[l], dst[l], cache_sem.at[len(cache)]))
            cache[-1].start()

    for copy in small[N_VEC:]:
        copy.wait()
    pos = pos_ref[...]
    posf = pos.astype(F32)
    posb[...] = jnp.broadcast_to(posf, posb.shape).astype(BF16)
    half = (8, SEQS)
    inv_freq = jnp.full(half, 1.0, F32)
    for i in range(1, 8):
        inv_freq = jnp.where(iota(half, 0) == i, F32(ROPE_BASE ** (-i / 8.0)), inv_freq)
    angle = jnp.broadcast_to(posf, half) * inv_freq
    cos_t = jnp.cos(angle)
    sin_t = jnp.sin(angle)

    b(VEC)
    b(0)
    b(1)
    c(VEC)
    c(0)
    a(3)
    b(2)
    d(VEC)
    e(VEC)

    vall = vecs[...].reshape(16, 8, LANES).astype(F32)
    wide_shape = (16, WIDTH)
    spread = jnp.where(iota((LANES, WIDTH), 0) % 32 == iota((LANES, WIDTH), 1) % 32, 1.0, 0.0).astype(BF16)
    own = iota(wide_shape, 1) // 32 == iota(wide_shape, 0)
    quarter = iota((16, LANES), 1) // 32
    qkv_shape = (LANES, 3 * WIDTH)
    spread_q = jnp.where(iota(qkv_shape, 0) == iota(qkv_shape, 1) % 96, 1.0, 0.0).astype(BF16)
    own_q = iota((16, 3 * WIDTH), 1) // 96 == iota((16, 3 * WIDTH), 0)

    def collapse(mask, part, table):
        return jnp.sum(jnp.where(mask, dot(part.astype(BF16), table), 0.0), axis=0, keepdims=True)

    for l in range(LAYERS):
        for k in range(7):
            part = jnp.where(quarter == k % 4, vall[:, 2 * (k // 4) + l, :], 0.0)
            lnp[l, k] = collapse(own, part, spread)
        bqkv[l] = collapse(own_q, vall[:, 4 + l, :], spread_q)
        share = vall[:, 6 + l, :]
        for n in range(8):
            bin_[l, n] = jnp.concatenate([share[2 * n:2 * n + 1], share[2 * n + 1:2 * n + 2]], axis=1)

    def rope(t):
        r1, r2 = t[:8], t[8:16]
        rot = jnp.concatenate([r1 * cos_t - r2 * sin_t, r2 * cos_t + r1 * sin_t, t[16:]], axis=0)
        return rot.astype(BF16)

    def qkv_stage(l):
        normed = normalize(hcur[...].astype(F32))
        h1 = (normed * lnp[l, 0] + lnp[l, 1]).astype(BF16)
        h2s[...] = (normed * lnp[l, 2] + lnp[l, 3]).astype(BF16)
        for j in range(HEADS // 2):
            cols = slice(PAIR * j, PAIR * (j + 1))
            y = dot(h1, whole(0, l)[:, :, :, :, :, cols].reshape(WIDTH, PAIR)) + bqkv[l][:, cols]
            yt = y.astype(BF16).astype(F32).T
            for g in range(2):
                q, k, v = (yt[HEAD * (3 * g + i):HEAD * (3 * g + i + 1)] for i in range(3))
                qs[2 * j + g] = rope(q).astype(F32) * (HEAD ** -0.5)
                kn[2 * j + g] = rope(k)
                vn[2 * j + g] = v.astype(BF16)

    def heads(l, h0, h1):
        def one_head(h, carry):
            def put(ref):
                def store(s, page):
                    ref[s, h] = page
                return store
            attend(h, pos, posb, qs, kn, vn, lambda s: ko[l][s, h], lambda s: vo[l][s, h],
                   put(ko[l]), put(vo[l]), sc, pr, ctxt)
            return carry

        lax.fori_loop(h0, h1, one_head, 0)

    c(1)
    d(0)
    a(4)
    b(3)
    e(0)
    c(2)
    qkv_stage(0)
    cache[0].wait()
    cache[1].wait()
    heads(0, 0, 4)
    a(5)
    b(4)
    d(1)
    heads(0, 4, 6)
    c(3)
    heads(0, 6, HEADS)
    accr[...] = attn_out(ctxt, wo0[...], lnp[0, 4])
    e(1)
    b(5)
    mlp_in(h2s, wi0, bin_, 0, act, 0, 4)
    d(2)
    mlp_in(h2s, wi0, bin_, 0, act, 4, 8)
    c(4)
    e(2)
    for j in range(2):
        cols = slice(SEQS * j, SEQS * (j + 1))
        m = dot(act[...], wd0[:, :, :, :, :, cols].reshape(FF, SEQS)) + lnp[0, 5][:, cols]
        hcur[:, cols] = (hcur[:, cols].astype(F32) + accr[:, cols] + m).astype(BF16)
    d(3)
    c(5)
    e(3)
    qkv_stage(1)
    cache[2].wait()
    cache[3].wait()
    heads(1, 0, EARLY)
    d(4)
    e(4)
    d(5)
    e(5)
    for copy in sends.values():
        copy.wait_send()


def finish_kernel(ko0, vo0, ko1, vo1, wo1, wi1, wd1, qs, kn, vn, ctxt, hcur, h2s, lnp, bin_, pos_ref,
                  out_hbm, k_hbm, v_hbm, kst, vst, ctxs, sc, pr, posb, act, outs, sems):
    last = LAYERS - 1
    copies = []

    def write(src, dst):
        copies.append(pltpu.make_async_copy(src, dst, sems.at[len(copies)]))
        copies[-1].start()

    for src, dst in ((ko0, k_hbm), (vo0, v_hbm)):
        for g in range(2):
            part = pl.ds(g * (SLOTS // 2), SLOTS // 2)
            write(src.at[part], dst.at[0, part])
    for src, dst in ((ko1, k_hbm), (vo1, v_hbm)):
        write(src.at[:, pl.ds(0, EARLY)], dst.at[last, :, pl.ds(0, EARLY)])
    pos = pos_ref[...]
    posb[...] = jnp.broadcast_to(pos.astype(F32), posb.shape).astype(BF16)
    ctxs[...] = ctxt[...]

    def put(ref, i):
        def store(s, page):
            ref[i, s] = page
        return store

    for i in range(HEADS - EARLY):
        h = EARLY + i
        attend(h, pos, posb, qs, kn, vn, lambda s: ko1[s, h], lambda s: vo1[s, h],
               put(kst, i), put(vst, i), sc, pr, ctxs)
        write(kst.at[i], k_hbm.at[last, :, h])
        write(vst.at[i], v_hbm.at[last, :, h])
    mlp_in(h2s, wi1, bin_, last, act, 0, 8)
    x = attn_out(ctxs, wo1[...], lnp[last, 4])
    m = dot(act[...], wd1[...].reshape(FF, WIDTH)) + lnp[last, 5]
    x = (hcur[...].astype(F32) + x + m).astype(BF16).astype(F32)
    outs[...] = (normalize(x) * lnp[0, 6] + lnp[1, 6]).astype(BF16)
    write(outs, out_hbm)
    for copy in copies:
        copy.wait()


def solution(mesh):
    row_spec = P('dp', None)
    vec_spec = P(None, 'dp')
    mat_spec = P(None, 'dp', None)
    cache_spec = P(None, 'dp', None, None, None)
    in_specs = (row_spec, P('dp'), cache_spec, cache_spec, vec_spec, vec_spec, vec_spec, vec_spec, mat_spec, vec_spec, mat_spec, vec_spec, mat_spec, vec_spec, mat_spec, vec_spec, P('dp'), P('dp'))
    out_specs = (row_spec, cache_spec, cache_spec)

    def device_step(x_embed, positions, k_cache, v_cache, ln1_gain, ln1_bias, ln2_gain, ln2_bias, w_qkv, b_qkv, w_out, b_out, w_in, b_in, w_down, b_down, lnf_gain, lnf_bias):
        vectors = (ln1_gain, ln1_bias, ln2_gain, ln2_bias, b_out, b_down, b_qkv, b_in,
                   lnf_gain.reshape(1, 32), lnf_bias.reshape(1, 32))
        to_lanes = (0, 2, 3, 4, 1)
        kt = jnp.transpose(k_cache, to_lanes)
        vt = jnp.transpose(v_cache, to_lanes)
        pos = positions.reshape(1, SEQS)
        vmem = pl.BlockSpec(memory_space=pltpu.VMEM)
        hbm = pl.BlockSpec(memory_space=pl.ANY)
        cache_shape = (LAYERS, SLOTS, HEADS, HEAD, SEQS)
        head_shape = (HEADS, HEAD, SEQS)
        out_w = GRID[1:] + (SLOTS, WIDTH)
        in_w = GRID[1:] + (SLOTS, FF)
        down_w = GRID[1:] + (LANES, WIDTH)
        carried = [pltpu.VMEM(shape, dtype) for shape, dtype in (
            *[(cache_shape[1:], BF16)] * 4, (out_w, BF16), (in_w, BF16), (down_w, BF16),
            (head_shape, F32), (head_shape, BF16), (head_shape, BF16), (head_shape, F32),
            ((SEQS, WIDTH), BF16), ((SEQS, WIDTH), BF16), ((LAYERS, 8, 1, WIDTH), F32),
            ((LAYERS, 8, 1, SEQS), F32), ((1, SEQS), jnp.int32))]
        state = pl.pallas_call(
            gather_kernel,
            out_shape=carried,
            in_specs=[hbm] * (8 + N_VEC),
            out_specs=[vmem] * len(carried),
            scratch_shapes=[
                pltpu.VMEM(GRID + (SLOTS, 3 * WIDTH), BF16),
                pltpu.VMEM(out_w, BF16),
                pltpu.VMEM(in_w, BF16),
                pltpu.VMEM(down_w, BF16),
                pltpu.VMEM(GRID[1:] + (8, LANES), BF16),
                pltpu.VMEM((LAYERS, 1, 3 * WIDTH), F32),
                pltpu.VMEM((SLOTS, SEQS), F32),
                pltpu.VMEM((SLOTS, SEQS), F32),
                pltpu.VMEM((SEQS, FF), BF16),
                pltpu.VMEM((SEQS, WIDTH), F32),
                pltpu.VMEM((16, SEQS), BF16),
                pltpu.SemaphoreType.DMA((8,)),
                pltpu.SemaphoreType.DMA((4,)),
                pltpu.SemaphoreType.DMA((2 + N_VEC,)),
                pltpu.SemaphoreType.DMA((len(ITEMS), 5)),
                pltpu.SemaphoreType.DMA((len(ITEMS), 5)),
                *[pltpu.VMEM(array.shape, BF16) for array in vectors],
            ],
            compiler_params=pltpu.CompilerParams(
                collective_id=0, has_side_effects=True, vmem_limit_bytes=SCOPED),
        )(x_embed, pos, *vectors, w_qkv, w_out, w_in, w_down, kt, vt)
        state = [pltpu.with_memory_space_constraint(array, pltpu.VMEM) for array in state]
        stage = pltpu.VMEM((HEADS - EARLY, SLOTS, HEAD, SEQS), BF16)
        out, ko, vo = pl.pallas_call(
            finish_kernel,
            out_shape=(pltpu.HBM((SEQS, WIDTH), BF16),
                       pltpu.HBM(cache_shape, BF16), pltpu.HBM(cache_shape, BF16)),
            in_specs=[vmem] * len(carried),
            out_specs=[pl.BlockSpec(memory_space=pltpu.HBM)] * 3,
            scratch_shapes=[
                stage, stage,
                pltpu.VMEM(head_shape, F32),
                pltpu.VMEM((SLOTS, SEQS), F32),
                pltpu.VMEM((SLOTS, SEQS), F32),
                pltpu.VMEM((16, SEQS), BF16),
                pltpu.VMEM((SEQS, FF), BF16),
                pltpu.VMEM((SEQS, WIDTH), BF16),
                pltpu.SemaphoreType.DMA((7 + 2 * (HEADS - EARLY),)),
            ],
            compiler_params=pltpu.CompilerParams(vmem_limit_bytes=SCOPED),
        )(*state)
        back = (0, 4, 1, 2, 3)
        return out, jnp.transpose(ko, back), jnp.transpose(vo, back)

    return jax.shard_map(device_step, mesh=mesh, in_specs=in_specs, out_specs=out_specs, check_vma=False)
```

```python
import jax
import jax.numpy as jnp
from jax import lax
from jax.experimental import pallas as pl
from jax.experimental.pallas import tpu as pltpu
from jax.sharding import PartitionSpec as P

LN_EPS = 1e-5
ROPE_BASE = 10000.0
F32 = jnp.float32
BF16 = jnp.bfloat16
MESH = pl.DeviceIdType.MESH
GRID = (2,) * 5
LAYERS, SEQS, WIDTH, SLOTS, HEADS, HEAD, LANES, FF = 2, 256, 512, 32, 8, 64, 128, 2048
PAIR = 6 * HEAD
EARLY = 2
ALL = slice(None)
SCOPED = 20 * 2 ** 20

ERF_NUM = (-2.72614225801306e-10, 2.77068142495902e-08, -2.10102402082508e-06,
           -5.69250639462346e-05, -7.34990630326855e-04, -2.95459980854025e-03,
           -1.60960333262415e-02)
ERF_DEN = (-1.45660718464996e-05, -2.13374055278905e-04, -1.68282697438203e-03,
           -7.37332916720468e-03, -1.42647390514189e-02)


def horner(coefs, t):
    acc = jnp.full_like(t, coefs[0])
    for coef in coefs[1:]:
        acc = acc * t + coef
    return acc


def gelu(v):
    u = jnp.clip(v * (0.5 ** 0.5), -4.0, 4.0)
    t = u * u
    erf = u * horner(ERF_NUM, t) / horner(ERF_DEN, t)
    return 0.5 * v * (1.0 + erf)


def normalize(v):
    centered = v - jnp.mean(v, axis=-1, keepdims=True)
    var = jnp.mean(centered * centered, axis=-1, keepdims=True)
    return centered * lax.rsqrt(var + LN_EPS)


def dot(a, b):
    return jnp.dot(a, b, preferred_element_type=F32)


def iota(shape, axis):
    return lax.broadcasted_iota(jnp.int32, shape, axis)


def pieces(l):
    rows = (l, 0, SLOTS)
    third = 5 * LANES
    qo = [(0, *rows, 0, third, 0), (0, *rows, third, third, 1),
          (0, *rows, 2 * third, 2 * LANES, 2), (1, *rows, 0, WIDTH, 2)]
    up = [(2, *rows, 0, third, 0), (2, *rows, third, third, 1), (2, *rows, 2 * third, 6 * LANES, 2)]
    down = [(3, l, 0, 48, 0, WIDTH, 0), (3, l, 48, 48, 0, WIDTH, 1), (3, l, 96, SLOTS, 0, WIDTH, 2)]
    return [qo, up, down]


PIECES = pieces(0) + pieces(1) + [[(4, 0, 0, HEADS, 0, LANES, 0)]]
VEC = len(PIECES) - 1
N_VEC = 10
ITEMS = [item for piece in PIECES for item in piece]
KEYS = list(dict.fromkeys(item[:2] for item in ITEMS))
FIRST = [sum(len(piece) for piece in PIECES[:p]) for p in range(len(PIECES) + 1)]


def attend(h, pos, posb, qs, kn, vn, k_in, v_in, k_out, v_out, sc, pr, ctxt):
    tiles = (HEAD // 16, 16, SEQS)
    knew = kn[h].reshape(tiles)
    vnew = vn[h].reshape(tiles)

    def insert(src, dst, s, new):
        mask = posb[...] == s.astype(BF16)
        page = jnp.where(mask[None], new, src(s).reshape(tiles)).reshape(HEAD, SEQS)
        dst(s, page)
        return page.astype(F32)

    def score(s, carry):
        page = insert(k_in, k_out, s, knew)
        sc[pl.ds(s, 1), :] = jnp.sum(page * qs[h], axis=0, keepdims=True)
        return carry

    lax.fori_loop(0, SLOTS, score, 0, unroll=8)
    sm = jnp.where(iota((SLOTS, SEQS), 0) <= pos, sc[...], -jnp.inf)
    ex = jnp.exp(sm - jnp.max(sm, axis=0, keepdims=True))
    probs = ex / jnp.sum(ex, axis=0, keepdims=True)
    pr[...] = probs.astype(BF16).astype(F32)

    def mix(s, acc):
        page = insert(v_in, v_out, s, vnew)
        return acc + page * pr[pl.ds(s, 1), :]

    ctx = lax.fori_loop(0, SLOTS, mix, jnp.zeros((HEAD, SEQS), F32), unroll=8)
    ctxt[h] = ctx.astype(BF16).astype(F32)


def attn_out(ctxt, w, bias):
    ctx = ctxt[...].reshape(WIDTH, SEQS).T.astype(BF16)
    return dot(ctx, w.reshape(WIDTH, WIDTH)) + bias


def mlp_in(h, w_ref, bias_ref, l, act, n0, n1):
    for n in range(n0, n1):
        cols = slice(n * SEQS, (n + 1) * SEQS)
        w = w_ref[:, :, :, :, :, cols].reshape(WIDTH, SEQS)
        act[:, cols] = gelu(dot(h[...], w) + bias_ref[l, n]).astype(BF16)


def gather_kernel(x_in, pos_in, *refs):
    gather_body(x_in, pos_in, refs[:N_VEC], *refs[N_VEC:-N_VEC], refs[-N_VEC:])


def gather_body(x_in, pos_in, vec_in, wq_in, wo_in, wi_in, wd_in, kc_in, vc_in,
                  ko0, vo0, ko1, vo1, wo1, wi1, wd1, qs, kn, vn, ctxt, hcur, h2s, lnp, bin_, pos_ref,
                  wq, wo0, wi0, wd0, vecs, bqkv, sc, pr, act, accr, posb,
                  local_sem, cache_sem, small_sem, send_sem, recv_sem, vec_ref):
    me = lax.axis_index('dp')
    core = me % 2
    px = (me // 2) % 2
    py = (me // 4) % 2
    pz = me // 8
    place = (px, py, pz)
    peer_core = me + 1 - 2 * core
    peers = (me + 2 - 4 * px, me + 4 - 8 * py, me + 8 - 16 * pz)
    shards = (wq_in, wo_in, wi_in, wd_in)

    def whole(m, l):
        if m == 4:
            return vecs
        return ((wq.at[0], wo0, wi0, wd0), (wq.at[1], wo1, wi1, wd1))[l][m]

    local = {}
    for l, m in [(l, m) for l in range(LAYERS) for m in range(4)]:
        local[(m, l)] = pltpu.make_async_copy(
            shards[m].at[l], whole(m, l).at[pz, py, px, core], local_sem.at[len(local)])
    for m in range(2):
        local[(m, 0)].start()
    barrier = pltpu.get_barrier_semaphore()
    for peer in peers + (peer_core,):
        pl.semaphore_signal(barrier, inc=1, device_id=(peer,), device_id_type=MESH)
    small = []
    for src, dst in zip((*vec_in, pos_in, x_in), (*vec_ref, pos_ref, hcur)):
        small.append(pltpu.make_async_copy(src, dst, small_sem.at[len(small)]))
        small[-1].start()
    for key, copy in local.items():
        if key not in ((0, 0), (1, 0)):
            copy.start()
    pl.semaphore_wait(barrier, len(peers) + 1)

    started = []

    def remote(ref, key, stage, peer):
        k = KEYS.index(key)
        return pltpu.make_async_remote_copy(
            src_ref=ref, dst_ref=ref, send_sem=send_sem.at[k, stage],
            recv_sem=recv_sem.at[k, stage], device_id=(peer,), device_id_type=MESH)

    def parts(key, stage):
        at = ([pz, py, px], [pz, py, ALL], [pz, ALL, ALL])[min(stage, 2)]
        return remote(whole(*key).at[(*at, core)], key, stage, peer_core)

    def landed(p, stage):
        for key in keys(p):
            parts(key, stage).wait_recv()
            yield from (i for i in ids(p) if ITEMS[i][:2] == key)

    def send(i, stage):
        m, l, r0, rn, c0, cn, o = ITEMS[i]
        axes = [(o + s) % 3 for s in range(3)]
        at = [place[2], place[1], place[0]]
        for ax in axes[:min(stage, 2)]:
            at[2 - ax] = ALL
        if stage == 4:
            at[2 - axes[2]] = 1 - place[axes[2]]
        ref = whole(m, l).at[(*at, core, pl.ds(r0, rn), pl.ds(c0, cn))]
        peer = peers[axes[stage]] if stage < 3 else peer_core
        remote(ref, (m, l), stage, peer).start()
        if ((m, l), stage) not in started:
            started.append(((m, l), stage))

    def ids(p):
        return range(FIRST[p], FIRST[p + 1])

    def keys(p):
        return list(dict.fromkeys(ITEMS[i][:2] for i in ids(p)))

    def a(p):
        for key in keys(p):
            if key in local:
                local[key].wait()
        for i in ids(p):
            send(i, 0)

    def b(p):
        for i in landed(p, 0):
            send(i, 1)

    def c(p):
        for i in landed(p, 1):
            send(i, 2)
            send(i, 3)

    def d(p):
        for i in landed(p, 2):
            send(i, 4)

    def e(p):
        for stage in (3, 4):
            list(landed(p, stage))

    a(0)
    for copy in small[:N_VEC]:
        copy.wait()
    g1, b1, g2, b2, bo, bd, bq, bi, gf, bf = (ref[...].astype(F32) for ref in vec_ref)
    pad = jnp.zeros((LAYERS, 32), F32)
    groups = ([g1, b1, g2, b2], [bo, bd, jnp.concatenate([gf, bf], axis=0), pad], [bq, pad])
    rows = [jnp.concatenate(group, axis=1) for group in groups] + [bi]
    vecs[pz, py, px, core] = jnp.concatenate(rows, axis=0).astype(BF16)
    a(VEC)
    a(1)
    a(2)
    cache = []
    ko, vo = (ko0, ko1), (vo0, vo1)
    for l in range(LAYERS):
        for src, dst in ((kc_in, ko), (vc_in, vo)):
            cache.append(pltpu.make_async_copy(src.at[l], dst[l], cache_sem.at[len(cache)]))
            cache[-1].start()

    for copy in small[N_VEC:]:
        copy.wait()
    pos = pos_ref[...]
    posf = pos.astype(F32)
    posb[...] = jnp.broadcast_to(posf, posb.shape).astype(BF16)
    half = (8, SEQS)
    inv_freq = jnp.full(half, 1.0, F32)
    for i in range(1, 8):
        inv_freq = jnp.where(iota(half, 0) == i, F32(ROPE_BASE ** (-i / 8.0)), inv_freq)
    angle = jnp.broadcast_to(posf, half) * inv_freq
    cos_t = jnp.cos(angle)
    sin_t = jnp.sin(angle)

    b(VEC)
    b(0)
    b(1)
    c(VEC)
    c(0)
    a(3)
    b(2)
    d(VEC)
    e(VEC)

    vall = vecs[...].reshape(16, 8, LANES).astype(F32)
    wide_shape = (16, WIDTH)
    spread = jnp.where(iota((LANES, WIDTH), 0) % 32 == iota((LANES, WIDTH), 1) % 32, 1.0, 0.0).astype(BF16)
    own = iota(wide_shape, 1) // 32 == iota(wide_shape, 0)
    quarter = iota((16, LANES), 1) // 32
    qkv_shape = (LANES, 3 * WIDTH)
    spread_q = jnp.where(iota(qkv_shape, 0) == iota(qkv_shape, 1) % 96, 1.0, 0.0).astype(BF16)
    own_q = iota((16, 3 * WIDTH), 1) // 96 == iota((16, 3 * WIDTH), 0)

    def collapse(mask, part, table):
        return jnp.sum(jnp.where(mask, dot(part.astype(BF16), table), 0.0), axis=0, keepdims=True)

    for l in range(LAYERS):
        for k in range(7):
            part = jnp.where(quarter == k % 4, vall[:, 2 * (k // 4) + l, :], 0.0)
            lnp[l, k] = collapse(own, part, spread)
        bqkv[l] = collapse(own_q, vall[:, 4 + l, :], spread_q)
        share = vall[:, 6 + l, :]
        for n in range(8):
            bin_[l, n] = jnp.concatenate([share[2 * n:2 * n + 1], share[2 * n + 1:2 * n + 2]], axis=1)

    def rope(t):
        r1, r2 = t[:8], t[8:16]
        rot = jnp.concatenate([r1 * cos_t - r2 * sin_t, r2 * cos_t + r1 * sin_t, t[16:]], axis=0)
        return rot.astype(BF16)

    def qkv_stage(l):
        normed = normalize(hcur[...].astype(F32))
        h1 = (normed * lnp[l, 0] + lnp[l, 1]).astype(BF16)
        h2s[...] = (normed * lnp[l, 2] + lnp[l, 3]).astype(BF16)
        for j in range(HEADS // 2):
            cols = slice(PAIR * j, PAIR * (j + 1))
            y = dot(h1, whole(0, l)[:, :, :, :, :, cols].reshape(WIDTH, PAIR)) + bqkv[l][:, cols]
            yt = y.astype(BF16).astype(F32).T
            for g in range(2):
                q, k, v = (yt[HEAD * (3 * g + i):HEAD * (3 * g + i + 1)] for i in range(3))
                qs[2 * j + g] = rope(q).astype(F32) * (HEAD ** -0.5)
                kn[2 * j + g] = rope(k)
                vn[2 * j + g] = v.astype(BF16)

    def heads(l, h0, h1):
        def one_head(h, carry):
            def put(ref):
                def store(s, page):
                    ref[s, h] = page
                return store
            attend(h, pos, posb, qs, kn, vn, lambda s: ko[l][s, h], lambda s: vo[l][s, h],
                   put(ko[l]), put(vo[l]), sc, pr, ctxt)
            return carry

        lax.fori_loop(h0, h1, one_head, 0)

    c(1)
    d(0)
    a(4)
    b(3)
    e(0)
    c(2)
    qkv_stage(0)
    cache[0].wait()
    cache[1].wait()
    heads(0, 0, 4)
    a(5)
    b(4)
    d(1)
    heads(0, 4, 6)
    c(3)
    heads(0, 6, HEADS)
    accr[...] = attn_out(ctxt, wo0[...], lnp[0, 4])
    e(1)
    b(5)
    mlp_in(h2s, wi0, bin_, 0, act, 0, 4)
    d(2)
    mlp_in(h2s, wi0, bin_, 0, act, 4, 8)
    c(4)
    e(2)
    for j in range(2):
        cols = slice(SEQS * j, SEQS * (j + 1))
        m = dot(act[...], wd0[:, :, :, :, :, cols].reshape(FF, SEQS)) + lnp[0, 5][:, cols]
        hcur[:, cols] = (hcur[:, cols].astype(F32) + accr[:, cols] + m).astype(BF16)
    d(3)
    c(5)
    e(3)
    qkv_stage(1)
    cache[2].wait()
    cache[3].wait()
    heads(1, 0, EARLY)
    d(4)
    e(4)
    d(5)
    e(5)
    for key, stage in started:
        parts(key, stage).wait_send()


def finish_kernel(ko0, vo0, ko1, vo1, wo1, wi1, wd1, qs, kn, vn, ctxt, hcur, h2s, lnp, bin_, pos_ref,
                  out_hbm, k_hbm, v_hbm, kst, vst, ctxs, sc, pr, posb, act, outs, sems):
    last = LAYERS - 1
    copies = []

    def write(src, dst):
        copies.append(pltpu.make_async_copy(src, dst, sems.at[len(copies)]))
        copies[-1].start()

    for src, dst in ((ko0, k_hbm), (vo0, v_hbm)):
        for g in range(2):
            part = pl.ds(g * (SLOTS // 2), SLOTS // 2)
            write(src.at[part], dst.at[0, part])
    for src, dst in ((ko1, k_hbm), (vo1, v_hbm)):
        write(src.at[:, pl.ds(0, EARLY)], dst.at[last, :, pl.ds(0, EARLY)])
    pos = pos_ref[...]
    posb[...] = jnp.broadcast_to(pos.astype(F32), posb.shape).astype(BF16)
    ctxs[...] = ctxt[...]

    def put(ref, i):
        def store(s, page):
            ref[i, s] = page
        return store

    for i in range(HEADS - EARLY):
        h = EARLY + i
        attend(h, pos, posb, qs, kn, vn, lambda s: ko1[s, h], lambda s: vo1[s, h],
               put(kst, i), put(vst, i), sc, pr, ctxs)
        write(kst.at[i], k_hbm.at[last, :, h])
        write(vst.at[i], v_hbm.at[last, :, h])
    mlp_in(h2s, wi1, bin_, last, act, 0, 8)
    x = attn_out(ctxs, wo1[...], lnp[last, 4])
    m = dot(act[...], wd1[...].reshape(FF, WIDTH)) + lnp[last, 5]
    x = (hcur[...].astype(F32) + x + m).astype(BF16).astype(F32)
    outs[...] = (normalize(x) * lnp[0, 6] + lnp[1, 6]).astype(BF16)
    write(outs, out_hbm)
    for copy in copies:
        copy.wait()


def solution(mesh):
    row_spec = P('dp', None)
    vec_spec = P(None, 'dp')
    mat_spec = P(None, 'dp', None)
    cache_spec = P(None, 'dp', None, None, None)
    in_specs = (row_spec, P('dp'), cache_spec, cache_spec, vec_spec, vec_spec, vec_spec, vec_spec, mat_spec, vec_spec, mat_spec, vec_spec, mat_spec, vec_spec, mat_spec, vec_spec, P('dp'), P('dp'))
    out_specs = (row_spec, cache_spec, cache_spec)

    def device_step(x_embed, positions, k_cache, v_cache, ln1_gain, ln1_bias, ln2_gain, ln2_bias, w_qkv, b_qkv, w_out, b_out, w_in, b_in, w_down, b_down, lnf_gain, lnf_bias):
        vectors = (ln1_gain, ln1_bias, ln2_gain, ln2_bias, b_out, b_down, b_qkv, b_in,
                   lnf_gain.reshape(1, 32), lnf_bias.reshape(1, 32))
        to_lanes = (0, 2, 3, 4, 1)
        kt = jnp.transpose(k_cache, to_lanes)
        vt = jnp.transpose(v_cache, to_lanes)
        pos = positions.reshape(1, SEQS)
        vmem = pl.BlockSpec(memory_space=pltpu.VMEM)
        hbm = pl.BlockSpec(memory_space=pl.ANY)
        cache_shape = (LAYERS, SLOTS, HEADS, HEAD, SEQS)
        head_shape = (HEADS, HEAD, SEQS)
        out_w = GRID[1:] + (SLOTS, WIDTH)
        in_w = GRID[1:] + (SLOTS, FF)
        down_w = GRID[1:] + (LANES, WIDTH)
        carried = [pltpu.VMEM(shape, dtype) for shape, dtype in (
            *[(cache_shape[1:], BF16)] * 4, (out_w, BF16), (in_w, BF16), (down_w, BF16),
            (head_shape, F32), (head_shape, BF16), (head_shape, BF16), (head_shape, F32),
            ((SEQS, WIDTH), BF16), ((SEQS, WIDTH), BF16), ((LAYERS, 8, 1, WIDTH), F32),
            ((LAYERS, 8, 1, SEQS), F32), ((1, SEQS), jnp.int32))]
        state = pl.pallas_call(
            gather_kernel,
            out_shape=carried,
            in_specs=[hbm] * (8 + N_VEC),
            out_specs=[vmem] * len(carried),
            scratch_shapes=[
                pltpu.VMEM(GRID + (SLOTS, 3 * WIDTH), BF16),
                pltpu.VMEM(out_w, BF16),
                pltpu.VMEM(in_w, BF16),
                pltpu.VMEM(down_w, BF16),
                pltpu.VMEM(GRID[1:] + (8, LANES), BF16),
                pltpu.VMEM((LAYERS, 1, 3 * WIDTH), F32),
                pltpu.VMEM((SLOTS, SEQS), F32),
                pltpu.VMEM((SLOTS, SEQS), F32),
                pltpu.VMEM((SEQS, FF), BF16),
                pltpu.VMEM((SEQS, WIDTH), F32),
                pltpu.VMEM((16, SEQS), BF16),
                pltpu.SemaphoreType.DMA((8,)),
                pltpu.SemaphoreType.DMA((4,)),
                pltpu.SemaphoreType.DMA((2 + N_VEC,)),
                pltpu.SemaphoreType.DMA((len(KEYS), 5)),
                pltpu.SemaphoreType.DMA((len(KEYS), 5)),
                *[pltpu.VMEM(array.shape, BF16) for array in vectors],
            ],
            compiler_params=pltpu.CompilerParams(
                collective_id=0, has_side_effects=True, vmem_limit_bytes=SCOPED),
        )(x_embed, pos, *vectors, w_qkv, w_out, w_in, w_down, kt, vt)
        state = [pltpu.with_memory_space_constraint(array, pltpu.VMEM) for array in state]
        stage = pltpu.VMEM((HEADS - EARLY, SLOTS, HEAD, SEQS), BF16)
        out, ko, vo = pl.pallas_call(
            finish_kernel,
            out_shape=(pltpu.HBM((SEQS, WIDTH), BF16),
                       pltpu.HBM(cache_shape, BF16), pltpu.HBM(cache_shape, BF16)),
            in_specs=[vmem] * len(carried),
            out_specs=[pl.BlockSpec(memory_space=pltpu.HBM)] * 3,
            scratch_shapes=[
                stage, stage,
                pltpu.VMEM(head_shape, F32),
                pltpu.VMEM((SLOTS, SEQS), F32),
                pltpu.VMEM((SLOTS, SEQS), F32),
                pltpu.VMEM((16, SEQS), BF16),
                pltpu.VMEM((SEQS, FF), BF16),
                pltpu.VMEM((SEQS, WIDTH), BF16),
                pltpu.SemaphoreType.DMA((7 + 2 * (HEADS - EARLY),)),
            ],
            compiler_params=pltpu.CompilerParams(vmem_limit_bytes=SCOPED),
        )(*state)
        back = (0, 4, 1, 2, 3)
        return out, jnp.transpose(ko, back), jnp.transpose(vo, back)

    return jax.shard_map(device_step, mesh=mesh, in_specs=in_specs, out_specs=out_specs, check_vma=False)
```

```python
import jax
import jax.numpy as jnp
from jax import lax
from jax.experimental import pallas as pl
from jax.experimental.pallas import tpu as pltpu
from jax.sharding import PartitionSpec as P

LN_EPS = 1e-5
ROPE_BASE = 10000.0
F32 = jnp.float32
BF16 = jnp.bfloat16
MESH = pl.DeviceIdType.MESH
GRID = (2,) * 5
LAYERS, SEQS, WIDTH, SLOTS, HEADS, HEAD, LANES, FF = 2, 256, 512, 32, 8, 64, 128, 2048
PAIR = 6 * HEAD
EARLY = 2
ALL = slice(None)
SCOPED = 19 * 2 ** 20

ERF_NUM = (-2.72614225801306e-10, 2.77068142495902e-08, -2.10102402082508e-06,
           -5.69250639462346e-05, -7.34990630326855e-04, -2.95459980854025e-03,
           -1.60960333262415e-02)
ERF_DEN = (-1.45660718464996e-05, -2.13374055278905e-04, -1.68282697438203e-03,
           -7.37332916720468e-03, -1.42647390514189e-02)


def horner(coefs, t):
    acc = jnp.full_like(t, coefs[0])
    for coef in coefs[1:]:
        acc = acc * t + coef
    return acc


def gelu(v):
    u = jnp.clip(v * (0.5 ** 0.5), -4.0, 4.0)
    t = u * u
    erf = u * horner(ERF_NUM, t) / horner(ERF_DEN, t)
    return 0.5 * v * (1.0 + erf)


def normalize(v):
    centered = v - jnp.mean(v, axis=-1, keepdims=True)
    var = jnp.mean(centered * centered, axis=-1, keepdims=True)
    return centered * lax.rsqrt(var + LN_EPS)


def dot(a, b):
    return jnp.dot(a, b, preferred_element_type=F32)


def iota(shape, axis):
    return lax.broadcasted_iota(jnp.int32, shape, axis)


QKV = 3 * WIDTH
WEIGHTS = 3


def pieces(l):
    third = 5 * LANES
    cols = ((0, third, 0), (third, third, 1), (2 * third, 6 * LANES, 2))
    down = [(2, l, 0, 48, 0, WIDTH, 0), (2, l, 48, 48, 0, WIDTH, 1), (2, l, 96, SLOTS, 0, WIDTH, 2)]
    return [[(m, l, 0, SLOTS, *c) for c in cols] for m in range(2)] + [down]


PIECES = pieces(0) + pieces(1) + [[(WEIGHTS, 0, 0, HEADS, 0, LANES, 0)]]
VEC = len(PIECES) - 1
N_VEC = 10
ITEMS = [item for piece in PIECES for item in piece]
KEYS = list(dict.fromkeys(item[:2] for item in ITEMS))
FIRST = [sum(len(piece) for piece in PIECES[:p]) for p in range(len(PIECES) + 1)]


def attend(h, pos, posb, qs, kn, vn, k_in, v_in, k_out, v_out, sc, pr, ctxt):
    tiles = (HEAD // 16, 16, SEQS)
    knew = kn[h].reshape(tiles)
    vnew = vn[h].reshape(tiles)

    def insert(src, dst, s, new):
        mask = posb[...] == s.astype(BF16)
        page = jnp.where(mask[None], new, src(s).reshape(tiles)).reshape(HEAD, SEQS)
        dst(s, page)
        return page.astype(F32)

    def score(s, carry):
        page = insert(k_in, k_out, s, knew)
        sc[pl.ds(s, 1), :] = jnp.sum(page * qs[h], axis=0, keepdims=True)
        return carry

    lax.fori_loop(0, SLOTS, score, 0, unroll=8)
    sm = jnp.where(iota((SLOTS, SEQS), 0) <= pos, sc[...], -jnp.inf)
    ex = jnp.exp(sm - jnp.max(sm, axis=0, keepdims=True))
    probs = ex / jnp.sum(ex, axis=0, keepdims=True)
    pr[...] = probs.astype(BF16).astype(F32)

    def mix(s, acc):
        page = insert(v_in, v_out, s, vnew)
        return acc + page * pr[pl.ds(s, 1), :]

    ctx = lax.fori_loop(0, SLOTS, mix, jnp.zeros((HEAD, SEQS), F32), unroll=8)
    ctxt[h] = ctx.astype(BF16).astype(F32)


def attn_out(ctxt, w_ref, bias):
    ctx = ctxt[...].reshape(WIDTH, SEQS).T.astype(BF16)
    return dot(ctx, w_ref[:, :, :, :, :, QKV:].reshape(WIDTH, WIDTH)) + bias


def mlp_in(h, w_ref, bias_ref, l, act, n0, n1):
    for n in range(n0, n1):
        cols = slice(n * SEQS, (n + 1) * SEQS)
        w = w_ref[:, :, :, :, :, cols].reshape(WIDTH, SEQS)
        act[:, cols] = gelu(dot(h[...], w) + bias_ref[l, n]).astype(BF16)


def gather_kernel(x_in, pos_in, *refs):
    gather_body(x_in, pos_in, refs[:N_VEC], *refs[N_VEC:-N_VEC], refs[-N_VEC:])


def gather_body(x_in, pos_in, vec_in, wq_in, wo_in, wi_in, wd_in, kc_in, vc_in,
                  ko0, vo0, ko1, vo1, wqo1, wi1, wd1, qs, kn, vn, ctxt, hcur, h2s, lnp, bin_, pos_ref,
                  wqo0, wi0, wd0, vecs, bqkv, sc, pr, act, accr, posb,
                  local_sem, cache_sem, small_sem, send_sem, recv_sem, vec_ref):
    me = lax.axis_index('dp')
    core = me % 2
    px = (me // 2) % 2
    py = (me // 4) % 2
    pz = me // 8
    place = (px, py, pz)
    peer_core = me + 1 - 2 * core
    peers = (me + 2 - 4 * px, me + 4 - 8 * py, me + 8 - 16 * pz)

    def whole(m, l):
        if m == WEIGHTS:
            return vecs
        return ((wqo0, wi0, wd0), (wqo1, wi1, wd1))[l][m]

    def place_own(m, l):
        own = whole(m, l).at[pz, py, px, core]
        sem = local_sem.at[m, l]
        parts_in = [((wi_in, wd_in)[m - 1].at[l], own)]
        if m == 0:
            parts_in = [(wq_in.at[l], own.at[:, pl.ds(0, QKV)]), (wo_in.at[l], own.at[:, pl.ds(QKV, WIDTH)])]
        for src, dst in parts_in:
            pltpu.make_async_copy(src, dst, sem).start()

    place_own(0, 0)
    barrier = pltpu.get_barrier_semaphore()
    for peer in peers + (peer_core,):
        pl.semaphore_signal(barrier, inc=1, device_id=(peer,), device_id_type=MESH)
    small = []
    for src, dst in zip((*vec_in, pos_in, x_in), (*vec_ref, pos_ref, hcur)):
        small.append(pltpu.make_async_copy(src, dst, small_sem.at[len(small)]))
        small[-1].start()
    for l in range(LAYERS):
        for m in range(WEIGHTS):
            if m + l:
                place_own(m, l)
    pl.semaphore_wait(barrier, len(peers) + 1)

    def remote(ref, key, stage, peer):
        k = KEYS.index(key)
        stage = min(stage, 3)
        return pltpu.make_async_remote_copy(
            src_ref=ref, dst_ref=ref, send_sem=send_sem.at[k // (LAYERS * WEIGHTS), stage],
            recv_sem=recv_sem.at[k, stage], device_id=(peer,), device_id_type=MESH)

    def parts(key, stage):
        at = ([pz, py, px], [pz, py, ALL], [pz, ALL, ALL], [ALL] * 3)[stage]
        return remote(whole(*key).at[(*at, core)], key, stage, peer_core)

    def landed(p, stage):
        for key in keys(p):
            parts(key, stage).wait_recv()
            yield from (i for i in ids(p) if ITEMS[i][:2] == key)

    def send(i, stage):
        m, l, r0, rn, c0, cn, o = ITEMS[i]
        axes = [(o + s) % 3 for s in range(3)]
        at = [place[2], place[1], place[0]]
        for ax in axes[:min(stage, 2)]:
            at[2 - ax] = ALL
        if stage == 4:
            at[2 - axes[2]] = 1 - place[axes[2]]
        ref = whole(m, l).at[(*at, core, pl.ds(r0, rn), pl.ds(c0, cn))]
        peer = peers[axes[stage]] if stage < 3 else peer_core
        remote(ref, (m, l), stage, peer).start()

    def ids(p):
        return range(FIRST[p], FIRST[p + 1])

    def keys(p):
        return list(dict.fromkeys(ITEMS[i][:2] for i in ids(p)))

    def a(p):
        for key in keys(p):
            m, l = key
            if m < WEIGHTS:
                own = whole(m, l).at[pz, py, px, core]
                pltpu.make_async_copy(own, own, local_sem.at[m, l]).wait()
        for i in ids(p):
            send(i, 0)

    def b(p):
        for i in landed(p, 0):
            send(i, 1)

    def c(p):
        for i in landed(p, 1):
            send(i, 2)
            send(i, 3)

    def d(p):
        for i in landed(p, 2):
            send(i, 4)

    def e(p):
        list(landed(p, 3))

    a(0)
    for copy in small[:N_VEC]:
        copy.wait()
    g1, b1, g2, b2, bo, bd, bq, bi, gf, bf = (ref[...].astype(F32) for ref in vec_ref)
    pad = jnp.zeros((LAYERS, 32), F32)
    groups = ([g1, b1, g2, b2], [bo, bd, jnp.concatenate([gf, bf], axis=0), pad], [bq, pad])
    rows = [jnp.concatenate(group, axis=1) for group in groups] + [bi]
    vecs[pz, py, px, core] = jnp.concatenate(rows, axis=0).astype(BF16)
    a(VEC)
    a(1)
    a(2)
    cache = []
    ko, vo = (ko0, ko1), (vo0, vo1)
    for l in range(LAYERS):
        for src, dst in ((kc_in, ko), (vc_in, vo)):
            cache.append(pltpu.make_async_copy(src.at[l], dst[l], cache_sem.at[len(cache)]))
            cache[-1].start()

    for copy in small[N_VEC:]:
        copy.wait()
    pos = pos_ref[...]
    posf = pos.astype(F32)
    posb[...] = jnp.broadcast_to(posf, posb.shape).astype(BF16)
    half = (8, SEQS)
    inv_freq = jnp.full(half, 1.0, F32)
    for i in range(1, 8):
        inv_freq = jnp.where(iota(half, 0) == i, F32(ROPE_BASE ** (-i / 8.0)), inv_freq)
    angle = jnp.broadcast_to(posf, half) * inv_freq
    cos_t = jnp.cos(angle)
    sin_t = jnp.sin(angle)

    b(VEC)
    b(0)
    b(1)
    c(VEC)
    c(0)
    a(3)
    b(2)
    d(VEC)
    e(VEC)

    vall = vecs[...].reshape(16, 8, LANES).astype(F32)
    wide_shape = (16, WIDTH)
    spread = jnp.where(iota((LANES, WIDTH), 0) % 32 == iota((LANES, WIDTH), 1) % 32, 1.0, 0.0).astype(BF16)
    own = iota(wide_shape, 1) // 32 == iota(wide_shape, 0)
    quarter = iota((16, LANES), 1) // 32
    qkv_shape = (LANES, 3 * WIDTH)
    spread_q = jnp.where(iota(qkv_shape, 0) == iota(qkv_shape, 1) % 96, 1.0, 0.0).astype(BF16)
    own_q = iota((16, 3 * WIDTH), 1) // 96 == iota((16, 3 * WIDTH), 0)

    def collapse(mask, part, table):
        return jnp.sum(jnp.where(mask, dot(part.astype(BF16), table), 0.0), axis=0, keepdims=True)

    for l in range(LAYERS):
        for k in range(7):
            part = jnp.where(quarter == k % 4, vall[:, 2 * (k // 4) + l, :], 0.0)
            lnp[l, k] = collapse(own, part, spread)
        bqkv[l] = collapse(own_q, vall[:, 4 + l, :], spread_q)
        share = vall[:, 6 + l, :]
        for n in range(8):
            bin_[l, n] = jnp.concatenate([share[2 * n:2 * n + 1], share[2 * n + 1:2 * n + 2]], axis=1)

    def rope(t):
        r1, r2 = t[:8], t[8:16]
        rot = jnp.concatenate([r1 * cos_t - r2 * sin_t, r2 * cos_t + r1 * sin_t, t[16:]], axis=0)
        return rot.astype(BF16)

    def qkv_stage(l):
        normed = normalize(hcur[...].astype(F32))
        h1 = (normed * lnp[l, 0] + lnp[l, 1]).astype(BF16)
        h2s[...] = (normed * lnp[l, 2] + lnp[l, 3]).astype(BF16)
        for j in range(HEADS // 2):
            cols = slice(PAIR * j, PAIR * (j + 1))
            y = dot(h1, whole(0, l)[:, :, :, :, :, cols].reshape(WIDTH, PAIR)) + bqkv[l][:, cols]
            yt = y.astype(BF16).astype(F32).T
            for g in range(2):
                q, k, v = (yt[HEAD * (3 * g + i):HEAD * (3 * g + i + 1)] for i in range(3))
                qs[2 * j + g] = rope(q).astype(F32) * (HEAD ** -0.5)
                kn[2 * j + g] = rope(k)
                vn[2 * j + g] = v.astype(BF16)

    def heads(l, h0, h1):
        def one_head(h, carry):
            def put(ref):
                def store(s, page):
                    ref[s, h] = page
                return store
            attend(h, pos, posb, qs, kn, vn, lambda s: ko[l][s, h], lambda s: vo[l][s, h],
                   put(ko[l]), put(vo[l]), sc, pr, ctxt)
            return carry

        lax.fori_loop(h0, h1, one_head, 0)

    c(1)
    d(0)
    a(4)
    b(3)
    e(0)
    c(2)
    qkv_stage(0)
    cache[0].wait()
    cache[1].wait()
    heads(0, 0, 4)
    a(5)
    b(4)
    d(1)
    heads(0, 4, 6)
    c(3)
    heads(0, 6, HEADS)
    accr[...] = attn_out(ctxt, wqo0, lnp[0, 4])
    e(1)
    b(5)
    mlp_in(h2s, wi0, bin_, 0, act, 0, 4)
    d(2)
    mlp_in(h2s, wi0, bin_, 0, act, 4, 8)
    c(4)
    e(2)
    for j in range(2):
        cols = slice(SEQS * j, SEQS * (j + 1))
        m = dot(act[...], wd0[:, :, :, :, :, cols].reshape(FF, SEQS)) + lnp[0, 5][:, cols]
        hcur[:, cols] = (hcur[:, cols].astype(F32) + accr[:, cols] + m).astype(BF16)
    d(3)
    c(5)
    e(3)
    qkv_stage(1)
    cache[2].wait()
    cache[3].wait()
    heads(1, 0, EARLY)
    d(4)
    e(4)
    d(5)
    e(5)
    for stage in range(4):
        pages = ko0.at[pl.ds(0, WEIGHTS * 2 ** stage)]
        remote(pages, KEYS[0], stage, peer_core).wait_send()
        parts(KEYS[-1], stage).wait_send()


def finish_kernel(ko0, vo0, ko1, vo1, wqo1, wi1, wd1, qs, kn, vn, ctxt, hcur, h2s, lnp, bin_, pos_ref,
                  out_hbm, k_hbm, v_hbm, kst, vst, ctxs, sc, pr, posb, act, outs, sems):
    last = LAYERS - 1
    outputs = (k_hbm, v_hbm, out_hbm)

    def write(src, n, *at):
        dst = outputs[n].at[at] if at else outputs[n]
        pltpu.make_async_copy(src, dst, sems.at[n]).start()

    for n, src in enumerate((ko0, vo0)):
        for g in range(2):
            part = pl.ds(g * (SLOTS // 2), SLOTS // 2)
            write(src.at[part], n, 0, part)
    for n, src in enumerate((ko1, vo1)):
        write(src.at[:, pl.ds(0, EARLY)], n, last, ALL, pl.ds(0, EARLY))
    pos = pos_ref[...]
    posb[...] = jnp.broadcast_to(pos.astype(F32), posb.shape).astype(BF16)
    ctxs[...] = ctxt[...]

    def put(ref, i):
        def store(s, page):
            ref[i, s] = page
        return store

    for i in range(HEADS - EARLY):
        h = EARLY + i
        attend(h, pos, posb, qs, kn, vn, lambda s: ko1[s, h], lambda s: vo1[s, h],
               put(kst, i), put(vst, i), sc, pr, ctxs)
        write(kst.at[i], 0, last, ALL, h)
        write(vst.at[i], 1, last, ALL, h)
    mlp_in(h2s, wi1, bin_, last, act, 0, 8)
    x = attn_out(ctxs, wqo1, lnp[last, 4])
    m = dot(act[...], wd1[...].reshape(FF, WIDTH)) + lnp[last, 5]
    x = (hcur[...].astype(F32) + x + m).astype(BF16).astype(F32)
    outs[...] = (normalize(x) * lnp[0, 6] + lnp[1, 6]).astype(BF16)
    write(outs, 2)
    for n, ref in enumerate(outputs):
        pltpu.make_async_copy(ref, ref, sems.at[n]).wait()


def solution(mesh):
    row_spec = P('dp', None)
    vec_spec = P(None, 'dp')
    mat_spec = P(None, 'dp', None)
    cache_spec = P(None, 'dp', None, None, None)
    in_specs = (row_spec, P('dp'), cache_spec, cache_spec, vec_spec, vec_spec, vec_spec, vec_spec, mat_spec, vec_spec, mat_spec, vec_spec, mat_spec, vec_spec, mat_spec, vec_spec, P('dp'), P('dp'))
    out_specs = (row_spec, cache_spec, cache_spec)

    def device_step(x_embed, positions, k_cache, v_cache, ln1_gain, ln1_bias, ln2_gain, ln2_bias, w_qkv, b_qkv, w_out, b_out, w_in, b_in, w_down, b_down, lnf_gain, lnf_bias):
        vectors = (ln1_gain, ln1_bias, ln2_gain, ln2_bias, b_out, b_down, b_qkv, b_in,
                   lnf_gain.reshape(1, 32), lnf_bias.reshape(1, 32))
        to_lanes = (0, 2, 3, 4, 1)
        kt = jnp.transpose(k_cache, to_lanes)
        vt = jnp.transpose(v_cache, to_lanes)
        pos = positions.reshape(1, SEQS)
        vmem = pl.BlockSpec(memory_space=pltpu.VMEM)
        hbm = pl.BlockSpec(memory_space=pl.ANY)
        cache_shape = (LAYERS, SLOTS, HEADS, HEAD, SEQS)
        head_shape = (HEADS, HEAD, SEQS)
        in_w = GRID[1:] + (SLOTS, FF)
        down_w = GRID[1:] + (LANES, WIDTH)
        carried = [pltpu.VMEM(shape, dtype) for shape, dtype in (
            *[(cache_shape[1:], BF16)] * 4, (in_w, BF16), (in_w, BF16), (down_w, BF16),
            (head_shape, F32), (head_shape, BF16), (head_shape, BF16), (head_shape, F32),
            ((SEQS, WIDTH), BF16), ((SEQS, WIDTH), BF16), ((LAYERS, 8, 1, WIDTH), F32),
            ((LAYERS, 8, 1, SEQS), F32), ((1, SEQS), jnp.int32))]
        state = pl.pallas_call(
            gather_kernel,
            out_shape=carried,
            in_specs=[hbm] * (8 + N_VEC),
            out_specs=[vmem] * len(carried),
            scratch_shapes=[
                pltpu.VMEM(in_w, BF16),
                pltpu.VMEM(in_w, BF16),
                pltpu.VMEM(down_w, BF16),
                pltpu.VMEM(GRID[1:] + (8, LANES), BF16),
                pltpu.VMEM((LAYERS, 1, 3 * WIDTH), F32),
                pltpu.VMEM((SLOTS, SEQS), F32),
                pltpu.VMEM((SLOTS, SEQS), F32),
                pltpu.VMEM((SEQS, FF), BF16),
                pltpu.VMEM((SEQS, WIDTH), F32),
                pltpu.VMEM((16, SEQS), BF16),
                pltpu.SemaphoreType.DMA((WEIGHTS, LAYERS)),
                pltpu.SemaphoreType.DMA((4,)),
                pltpu.SemaphoreType.DMA((2 + N_VEC,)),
                pltpu.SemaphoreType.DMA((LAYERS, 4)),
                pltpu.SemaphoreType.DMA((len(KEYS), 4)),
                *[pltpu.VMEM(array.shape, BF16) for array in vectors],
            ],
            compiler_params=pltpu.CompilerParams(
                collective_id=0, has_side_effects=True, vmem_limit_bytes=SCOPED),
        )(x_embed, pos, *vectors, w_qkv, w_out, w_in, w_down, kt, vt)
        state = [pltpu.with_memory_space_constraint(array, pltpu.VMEM) for array in state]
        stage = pltpu.VMEM((HEADS - EARLY, SLOTS, HEAD, SEQS), BF16)
        out, ko, vo = pl.pallas_call(
            finish_kernel,
            out_shape=(pltpu.HBM((SEQS, WIDTH), BF16),
                       pltpu.HBM(cache_shape, BF16), pltpu.HBM(cache_shape, BF16)),
            in_specs=[vmem] * len(carried),
            out_specs=[pl.BlockSpec(memory_space=pltpu.HBM)] * 3,
            scratch_shapes=[
                stage, stage,
                pltpu.VMEM(head_shape, F32),
                pltpu.VMEM((SLOTS, SEQS), F32),
                pltpu.VMEM((SLOTS, SEQS), F32),
                pltpu.VMEM((16, SEQS), BF16),
                pltpu.VMEM((SEQS, FF), BF16),
                pltpu.VMEM((SEQS, WIDTH), BF16),
                pltpu.SemaphoreType.DMA((3,)),
            ],
            compiler_params=pltpu.CompilerParams(vmem_limit_bytes=SCOPED),
        )(*state)
        back = (0, 4, 1, 2, 3)
        return out, jnp.transpose(ko, back), jnp.transpose(vo, back)

    return jax.shard_map(device_step, mesh=mesh, in_specs=in_specs, out_specs=out_specs, check_vma=False)
```

```python
import jax
import jax.numpy as jnp
from jax import lax
from jax.experimental import pallas as pl
from jax.experimental.pallas import tpu as pltpu
from jax.sharding import PartitionSpec as P

LN_EPS = 1e-5
ROPE_BASE = 10000.0
F32 = jnp.float32
BF16 = jnp.bfloat16
MESH = pl.DeviceIdType.MESH
GRID = (2,) * 5
LAYERS, SEQS, WIDTH, SLOTS, HEADS, HEAD, LANES, FF = 2, 256, 512, 32, 8, 64, 128, 2048
PAIR = 6 * HEAD
EARLY = 2
ALL = slice(None)
SCOPED = 19 * 2 ** 20

ERF_NUM = (-2.72614225801306e-10, 2.77068142495902e-08, -2.10102402082508e-06,
           -5.69250639462346e-05, -7.34990630326855e-04, -2.95459980854025e-03,
           -1.60960333262415e-02)
ERF_DEN = (-1.45660718464996e-05, -2.13374055278905e-04, -1.68282697438203e-03,
           -7.37332916720468e-03, -1.42647390514189e-02)


def horner(coefs, t):
    acc = jnp.full_like(t, coefs[0])
    for coef in coefs[1:]:
        acc = acc * t + coef
    return acc


def gelu(v):
    z = v * (0.5 ** 0.5)
    u = jnp.clip(z, -4.0, 4.0)
    t = u * u
    erf = u * horner(ERF_NUM, t) / horner(ERF_DEN, t)
    erf = jnp.where(z >= 4.0, 1.0, jnp.where(z <= -4.0, -1.0, erf))
    return 0.5 * v * (1.0 + erf)


def normalize(v):
    centered = v - jnp.mean(v, axis=-1, keepdims=True)
    var = jnp.mean(centered * centered, axis=-1, keepdims=True)
    return centered * lax.rsqrt(var + LN_EPS)


def dot(a, b):
    return jnp.dot(a, b, preferred_element_type=F32)


def iota(shape, axis):
    return lax.broadcasted_iota(jnp.int32, shape, axis)


QKV = 3 * WIDTH
WEIGHTS = 3


def pieces(l):
    third = 5 * LANES
    cols = ((0, third, 0), (third, third, 1), (2 * third, 6 * LANES, 2))
    down = [(2, l, 0, 48, 0, WIDTH, 0), (2, l, 48, 48, 0, WIDTH, 1), (2, l, 96, SLOTS, 0, WIDTH, 2)]
    return [[(m, l, 0, SLOTS, *c) for c in cols] for m in range(2)] + [down]


PIECES = pieces(0) + pieces(1) + [[(WEIGHTS, 0, 0, HEADS, 0, LANES, 0)]]
VEC = len(PIECES) - 1
N_VEC = 10
ITEMS = [item for piece in PIECES for item in piece]
KEYS = list(dict.fromkeys(item[:2] for item in ITEMS))
FIRST = [sum(len(piece) for piece in PIECES[:p]) for p in range(len(PIECES) + 1)]


def attend(h, pos, posb, qs, kn, vn, k_in, v_in, k_out, v_out, sc, pr, ctxt):
    tiles = (HEAD // 16, 16, SEQS)
    knew = kn[h].reshape(tiles)
    vnew = vn[h].reshape(tiles)

    def insert(src, dst, s, new):
        mask = posb[...] == s.astype(BF16)
        page = jnp.where(mask[None], new, src(s).reshape(tiles)).reshape(HEAD, SEQS)
        dst(s, page)
        return page.astype(F32)

    def score(s, carry):
        page = insert(k_in, k_out, s, knew)
        sc[pl.ds(s, 1), :] = jnp.sum(page * qs[h], axis=0, keepdims=True)
        return carry

    lax.fori_loop(0, SLOTS, score, 0, unroll=8)
    sm = jnp.where(iota((SLOTS, SEQS), 0) <= pos, sc[...], -jnp.inf)
    ex = jnp.exp(sm - jnp.max(sm, axis=0, keepdims=True))
    probs = ex / jnp.sum(ex, axis=0, keepdims=True)
    pr[...] = probs.astype(BF16).astype(F32)

    def mix(s, acc):
        page = insert(v_in, v_out, s, vnew)
        return acc + page * pr[pl.ds(s, 1), :]

    ctx = lax.fori_loop(0, SLOTS, mix, jnp.zeros((HEAD, SEQS), F32), unroll=8)
    ctxt[h] = ctx.astype(BF16).astype(F32)


def attn_out(ctxt, w_ref, bias):
    ctx = ctxt[...].reshape(WIDTH, SEQS).T.astype(BF16)
    return dot(ctx, w_ref[:, :, :, :, :, QKV:].reshape(WIDTH, WIDTH)) + bias


def mlp_in(h, w_ref, bias_ref, l, act, n0, n1):
    for n in range(n0, n1):
        cols = slice(n * SEQS, (n + 1) * SEQS)
        w = w_ref[:, :, :, :, :, cols].reshape(WIDTH, SEQS)
        act[:, cols] = gelu(dot(h[...], w) + bias_ref[l, n]).astype(BF16)


def gather_kernel(x_in, pos_in, *refs):
    gather_body(x_in, pos_in, refs[:N_VEC], *refs[N_VEC:-N_VEC], refs[-N_VEC:])


def gather_body(x_in, pos_in, vec_in, wq_in, wo_in, wi_in, wd_in, kc_in, vc_in,
                  ko0, vo0, ko1, vo1, wqo1, wi1, wd1, qs, kn, vn, ctxt, hcur, h2s, lnp, bin_, pos_ref,
                  wqo0, wi0, wd0, vecs, bqkv, sc, pr, act, accr, posb,
                  local_sem, cache_sem, small_sem, send_sem, recv_sem, vec_ref):
    me = lax.axis_index('dp')
    core = me % 2
    px = (me // 2) % 2
    py = (me // 4) % 2
    pz = me // 8
    place = (px, py, pz)
    peer_core = me + 1 - 2 * core
    peers = (me + 2 - 4 * px, me + 4 - 8 * py, me + 8 - 16 * pz)

    def whole(m, l):
        if m == WEIGHTS:
            return vecs
        return ((wqo0, wi0, wd0), (wqo1, wi1, wd1))[l][m]

    def place_own(m, l):
        own = whole(m, l).at[pz, py, px, core]
        sem = local_sem.at[m, l]
        parts_in = [((wi_in, wd_in)[m - 1].at[l], own)]
        if m == 0:
            parts_in = [(wq_in.at[l], own.at[:, pl.ds(0, QKV)]), (wo_in.at[l], own.at[:, pl.ds(QKV, WIDTH)])]
        for src, dst in parts_in:
            pltpu.make_async_copy(src, dst, sem).start()

    place_own(0, 0)
    barrier = pltpu.get_barrier_semaphore()
    for peer in peers + (peer_core,):
        pl.semaphore_signal(barrier, inc=1, device_id=(peer,), device_id_type=MESH)
    small = []
    for src, dst in zip((*vec_in, pos_in, x_in), (*vec_ref, pos_ref, hcur)):
        small.append(pltpu.make_async_copy(src, dst, small_sem.at[len(small)]))
        small[-1].start()
    for l in range(LAYERS):
        for m in range(WEIGHTS):
            if m + l:
                place_own(m, l)
    for copy in small[:N_VEC]:
        copy.wait()
    g1, b1, g2, b2, bo, bd, bq, bi, gf, bf = (ref[...].astype(F32) for ref in vec_ref)
    pad = jnp.zeros((LAYERS, 32), F32)
    groups = ([g1, b1, g2, b2], [bo, bd, jnp.concatenate([gf, bf], axis=0), pad], [bq, pad])
    rows = [jnp.concatenate(group, axis=1) for group in groups] + [bi]
    vecs[pz, py, px, core] = jnp.concatenate(rows, axis=0).astype(BF16)
    pl.semaphore_wait(barrier, len(peers) + 1)

    def remote(ref, key, stage, peer):
        k = KEYS.index(key)
        stage = min(stage, 3)
        return pltpu.make_async_remote_copy(
            src_ref=ref, dst_ref=ref, send_sem=send_sem.at[k // (LAYERS * WEIGHTS), stage],
            recv_sem=recv_sem.at[k, stage], device_id=(peer,), device_id_type=MESH)

    def parts(key, stage):
        at = ([pz, py, px], [pz, py, ALL], [pz, ALL, ALL], [ALL] * 3)[stage]
        return remote(whole(*key).at[(*at, core)], key, stage, peer_core)

    def landed(p, stage):
        for key in keys(p):
            parts(key, stage).wait_recv()
            yield from (i for i in ids(p) if ITEMS[i][:2] == key)

    def send(i, stage):
        m, l, r0, rn, c0, cn, o = ITEMS[i]
        axes = [(o + s) % 3 for s in range(3)]
        at = [place[2], place[1], place[0]]
        for ax in axes[:min(stage, 2)]:
            at[2 - ax] = ALL
        if stage == 4:
            at[2 - axes[2]] = 1 - place[axes[2]]
        ref = whole(m, l).at[(*at, core, pl.ds(r0, rn), pl.ds(c0, cn))]
        peer = peers[axes[stage]] if stage < 3 else peer_core
        remote(ref, (m, l), stage, peer).start()

    def ids(p):
        return range(FIRST[p], FIRST[p + 1])

    def keys(p):
        return list(dict.fromkeys(ITEMS[i][:2] for i in ids(p)))

    def a(p):
        for key in keys(p):
            m, l = key
            if m < WEIGHTS:
                own = whole(m, l).at[pz, py, px, core]
                pltpu.make_async_copy(own, own, local_sem.at[m, l]).wait()
        for i in ids(p):
            send(i, 0)

    def b(p):
        for i in landed(p, 0):
            send(i, 1)

    def c(p):
        for i in landed(p, 1):
            send(i, 2)
            send(i, 3)

    def d(p):
        for i in landed(p, 2):
            send(i, 4)

    def e(p):
        list(landed(p, 3))

    a(0)
    a(VEC)
    a(1)
    a(2)
    cache = []
    ko, vo = (ko0, ko1), (vo0, vo1)
    for l in range(LAYERS):
        for src, dst in ((kc_in, ko), (vc_in, vo)):
            cache.append(pltpu.make_async_copy(src.at[l], dst[l], cache_sem.at[len(cache)]))
            cache[-1].start()

    for copy in small[N_VEC:]:
        copy.wait()
    pos = pos_ref[...]
    posf = pos.astype(F32)
    posb[...] = jnp.broadcast_to(posf, posb.shape).astype(BF16)
    half = (8, SEQS)
    inv_freq = jnp.full(half, 1.0, F32)
    for i in range(1, 8):
        inv_freq = jnp.where(iota(half, 0) == i, F32(ROPE_BASE ** (-i / 8.0)), inv_freq)
    angle = jnp.broadcast_to(posf, half) * inv_freq
    cos_t = jnp.cos(angle)
    sin_t = jnp.sin(angle)

    b(VEC)
    b(0)
    b(1)
    c(VEC)
    c(0)
    a(3)
    b(2)
    d(VEC)
    e(VEC)

    vall = vecs[...].reshape(16, 8, LANES).astype(F32)
    wide_shape = (16, WIDTH)
    spread = jnp.where(iota((LANES, WIDTH), 0) % 32 == iota((LANES, WIDTH), 1) % 32, 1.0, 0.0).astype(BF16)
    own = iota(wide_shape, 1) // 32 == iota(wide_shape, 0)
    quarter = iota((16, LANES), 1) // 32
    qkv_shape = (LANES, 3 * WIDTH)
    spread_q = jnp.where(iota(qkv_shape, 0) == iota(qkv_shape, 1) % 96, 1.0, 0.0).astype(BF16)
    own_q = iota((16, 3 * WIDTH), 1) // 96 == iota((16, 3 * WIDTH), 0)

    def collapse(mask, part, table):
        return jnp.sum(jnp.where(mask, dot(part.astype(BF16), table), 0.0), axis=0, keepdims=True)

    for l in range(LAYERS):
        for k in range(7):
            part = jnp.where(quarter == k % 4, vall[:, 2 * (k // 4) + l, :], 0.0)
            lnp[l, k] = collapse(own, part, spread)
        bqkv[l] = collapse(own_q, vall[:, 4 + l, :], spread_q)
        share = vall[:, 6 + l, :]
        for n in range(8):
            bin_[l, n] = jnp.concatenate([share[2 * n:2 * n + 1], share[2 * n + 1:2 * n + 2]], axis=1)

    def rope(t):
        r1, r2 = t[:8], t[8:16]
        rot = jnp.concatenate([r1 * cos_t - r2 * sin_t, r2 * cos_t + r1 * sin_t, t[16:]], axis=0)
        return rot.astype(BF16)

    def qkv_stage(l):
        normed = normalize(hcur[...].astype(F32))
        h1 = (normed * lnp[l, 0] + lnp[l, 1]).astype(BF16)
        h2s[...] = (normed * lnp[l, 2] + lnp[l, 3]).astype(BF16)
        for j in range(HEADS // 2):
            cols = slice(PAIR * j, PAIR * (j + 1))
            y = dot(h1, whole(0, l)[:, :, :, :, :, cols].reshape(WIDTH, PAIR)) + bqkv[l][:, cols]
            yt = y.astype(BF16).astype(F32).T
            for g in range(2):
                q, k, v = (yt[HEAD * (3 * g + i):HEAD * (3 * g + i + 1)] for i in range(3))
                qs[2 * j + g] = rope(q).astype(F32) * (HEAD ** -0.5)
                kn[2 * j + g] = rope(k)
                vn[2 * j + g] = v.astype(BF16)

    def heads(l, h0, h1):
        def one_head(h, carry):
            def put(ref):
                def store(s, page):
                    ref[s, h] = page
                return store
            attend(h, pos, posb, qs, kn, vn, lambda s: ko[l][s, h], lambda s: vo[l][s, h],
                   put(ko[l]), put(vo[l]), sc, pr, ctxt)
            return carry

        lax.fori_loop(h0, h1, one_head, 0)

    c(1)
    d(0)
    a(4)
    b(3)
    e(0)
    c(2)
    qkv_stage(0)
    cache[0].wait()
    cache[1].wait()
    heads(0, 0, 4)
    a(5)
    b(4)
    d(1)
    heads(0, 4, 6)
    c(3)
    heads(0, 6, HEADS)
    accr[...] = attn_out(ctxt, wqo0, lnp[0, 4])
    e(1)
    b(5)
    mlp_in(h2s, wi0, bin_, 0, act, 0, 4)
    d(2)
    mlp_in(h2s, wi0, bin_, 0, act, 4, 8)
    c(4)
    e(2)
    for j in range(2):
        cols = slice(SEQS * j, SEQS * (j + 1))
        m = dot(act[...], wd0[:, :, :, :, :, cols].reshape(FF, SEQS)) + lnp[0, 5][:, cols]
        hcur[:, cols] = (hcur[:, cols].astype(F32) + accr[:, cols] + m).astype(BF16)
    d(3)
    c(5)
    e(3)
    qkv_stage(1)
    cache[2].wait()
    cache[3].wait()
    heads(1, 0, EARLY)
    d(4)
    e(4)
    d(5)
    e(5)
    for stage in range(4):
        pages = ko0.at[pl.ds(0, WEIGHTS * 2 ** stage)]
        remote(pages, KEYS[0], stage, peer_core).wait_send()
        parts(KEYS[-1], stage).wait_send()


def finish_kernel(ko0, vo0, ko1, vo1, wqo1, wi1, wd1, qs, kn, vn, ctxt, hcur, h2s, lnp, bin_, pos_ref,
                  out_hbm, k_hbm, v_hbm, kst, vst, ctxs, sc, pr, posb, act, outs, sems):
    last = LAYERS - 1
    outputs = (k_hbm, v_hbm, out_hbm)

    def write(src, n, *at):
        dst = outputs[n].at[at] if at else outputs[n]
        pltpu.make_async_copy(src, dst, sems.at[n]).start()

    for n, src in enumerate((ko0, vo0)):
        for g in range(2):
            part = pl.ds(g * (SLOTS // 2), SLOTS // 2)
            write(src.at[part], n, 0, part)
    for n, src in enumerate((ko1, vo1)):
        write(src.at[:, pl.ds(0, EARLY)], n, last, ALL, pl.ds(0, EARLY))
    pos = pos_ref[...]
    posb[...] = jnp.broadcast_to(pos.astype(F32), posb.shape).astype(BF16)
    ctxs[...] = ctxt[...]

    def put(ref, i):
        def store(s, page):
            ref[i, s] = page
        return store

    for i in range(HEADS - EARLY):
        h = EARLY + i
        attend(h, pos, posb, qs, kn, vn, lambda s: ko1[s, h], lambda s: vo1[s, h],
               put(kst, i), put(vst, i), sc, pr, ctxs)
        write(kst.at[i], 0, last, ALL, h)
        write(vst.at[i], 1, last, ALL, h)
    mlp_in(h2s, wi1, bin_, last, act, 0, 8)
    x = attn_out(ctxs, wqo1, lnp[last, 4])
    m = dot(act[...], wd1[...].reshape(FF, WIDTH)) + lnp[last, 5]
    x = (hcur[...].astype(F32) + x + m).astype(BF16).astype(F32)
    outs[...] = (normalize(x) * lnp[0, 6] + lnp[1, 6]).astype(BF16)
    write(outs, 2)
    for n, ref in enumerate(outputs):
        pltpu.make_async_copy(ref, ref, sems.at[n]).wait()


def solution(mesh):
    row_spec = P('dp', None)
    vec_spec = P(None, 'dp')
    mat_spec = P(None, 'dp', None)
    cache_spec = P(None, 'dp', None, None, None)
    in_specs = (row_spec, P('dp'), cache_spec, cache_spec, vec_spec, vec_spec, vec_spec, vec_spec, mat_spec, vec_spec, mat_spec, vec_spec, mat_spec, vec_spec, mat_spec, vec_spec, P('dp'), P('dp'))
    out_specs = (row_spec, cache_spec, cache_spec)

    def device_step(x_embed, positions, k_cache, v_cache, ln1_gain, ln1_bias, ln2_gain, ln2_bias, w_qkv, b_qkv, w_out, b_out, w_in, b_in, w_down, b_down, lnf_gain, lnf_bias):
        vectors = (ln1_gain, ln1_bias, ln2_gain, ln2_bias, b_out, b_down, b_qkv, b_in,
                   lnf_gain.reshape(1, 32), lnf_bias.reshape(1, 32))
        to_lanes = (0, 2, 3, 4, 1)
        kt = jnp.transpose(k_cache, to_lanes)
        vt = jnp.transpose(v_cache, to_lanes)
        pos = positions.reshape(1, SEQS)
        vmem = pl.BlockSpec(memory_space=pltpu.VMEM)
        hbm = pl.BlockSpec(memory_space=pl.ANY)
        cache_shape = (LAYERS, SLOTS, HEADS, HEAD, SEQS)
        head_shape = (HEADS, HEAD, SEQS)
        in_w = GRID[1:] + (SLOTS, FF)
        down_w = GRID[1:] + (LANES, WIDTH)
        carried = [pltpu.VMEM(shape, dtype) for shape, dtype in (
            *[(cache_shape[1:], BF16)] * 4, (in_w, BF16), (in_w, BF16), (down_w, BF16),
            (head_shape, F32), (head_shape, BF16), (head_shape, BF16), (head_shape, F32),
            ((SEQS, WIDTH), BF16), ((SEQS, WIDTH), BF16), ((LAYERS, 8, 1, WIDTH), F32),
            ((LAYERS, 8, 1, SEQS), F32), ((1, SEQS), jnp.int32))]
        state = pl.pallas_call(
            gather_kernel,
            out_shape=carried,
            in_specs=[hbm] * (8 + N_VEC),
            out_specs=[vmem] * len(carried),
            scratch_shapes=[
                pltpu.VMEM(in_w, BF16),
                pltpu.VMEM(in_w, BF16),
                pltpu.VMEM(down_w, BF16),
                pltpu.VMEM(GRID[1:] + (8, LANES), BF16),
                pltpu.VMEM((LAYERS, 1, 3 * WIDTH), F32),
                pltpu.VMEM((SLOTS, SEQS), F32),
                pltpu.VMEM((SLOTS, SEQS), F32),
                pltpu.VMEM((SEQS, FF), BF16),
                pltpu.VMEM((SEQS, WIDTH), F32),
                pltpu.VMEM((16, SEQS), BF16),
                pltpu.SemaphoreType.DMA((WEIGHTS, LAYERS)),
                pltpu.SemaphoreType.DMA((4,)),
                pltpu.SemaphoreType.DMA((2 + N_VEC,)),
                pltpu.SemaphoreType.DMA((LAYERS, 4)),
                pltpu.SemaphoreType.DMA((len(KEYS), 4)),
                *[pltpu.VMEM(array.shape, BF16) for array in vectors],
            ],
            compiler_params=pltpu.CompilerParams(
                collective_id=0, has_side_effects=True, vmem_limit_bytes=SCOPED),
        )(x_embed, pos, *vectors, w_qkv, w_out, w_in, w_down, kt, vt)
        state = [pltpu.with_memory_space_constraint(array, pltpu.VMEM) for array in state]
        stage = pltpu.VMEM((HEADS - EARLY, SLOTS, HEAD, SEQS), BF16)
        out, ko, vo = pl.pallas_call(
            finish_kernel,
            out_shape=(pltpu.HBM((SEQS, WIDTH), BF16),
                       pltpu.HBM(cache_shape, BF16), pltpu.HBM(cache_shape, BF16)),
            in_specs=[vmem] * len(carried),
            out_specs=[pl.BlockSpec(memory_space=pltpu.HBM)] * 3,
            scratch_shapes=[
                stage, stage,
                pltpu.VMEM(head_shape, F32),
                pltpu.VMEM((SLOTS, SEQS), F32),
                pltpu.VMEM((SLOTS, SEQS), F32),
                pltpu.VMEM((16, SEQS), BF16),
                pltpu.VMEM((SEQS, FF), BF16),
                pltpu.VMEM((SEQS, WIDTH), BF16),
                pltpu.SemaphoreType.DMA((3,)),
            ],
            compiler_params=pltpu.CompilerParams(vmem_limit_bytes=SCOPED),
        )(*state)
        back = (0, 4, 1, 2, 3)
        return out, jnp.transpose(ko, back), jnp.transpose(vo, back)

    return jax.shard_map(device_step, mesh=mesh, in_specs=in_specs, out_specs=out_specs, check_vma=False)
```

```python
import jax
import jax.numpy as jnp
from jax import lax
from jax.experimental import pallas as pl
from jax.experimental.pallas import tpu as pltpu
from jax.sharding import PartitionSpec as P

LN_EPS = 1e-5
ROPE_BASE = 10000.0
F32 = jnp.float32
BF16 = jnp.bfloat16
MESH = pl.DeviceIdType.MESH
GRID = (2,) * 5
LAYERS, SEQS, WIDTH, SLOTS, HEADS, HEAD, LANES, FF = 2, 256, 512, 32, 8, 64, 128, 2048
PAIR = 6 * HEAD
EARLY = 2
ALL = slice(None)
SCOPED = 19 * 2 ** 20

ERF_NUM = (-2.72614225801306e-10, 2.77068142495902e-08, -2.10102402082508e-06,
           -5.69250639462346e-05, -7.34990630326855e-04, -2.95459980854025e-03,
           -1.60960333262415e-02)
ERF_DEN = (-1.45660718464996e-05, -2.13374055278905e-04, -1.68282697438203e-03,
           -7.37332916720468e-03, -1.42647390514189e-02)


def horner(coefs, t):
    acc = jnp.full_like(t, coefs[0])
    for coef in coefs[1:]:
        acc = acc * t + coef
    return acc


def gelu(v):
    z = v * (0.5 ** 0.5)
    u = jnp.clip(z, -4.0, 4.0)
    t = u * u
    erf = u * horner(ERF_NUM, t) / horner(ERF_DEN, t)
    erf = jnp.where(z >= 4.0, 1.0, jnp.where(z <= -4.0, -1.0, erf))
    return 0.5 * v * (1.0 + erf)


def normalize(v):
    centered = v - jnp.mean(v, axis=-1, keepdims=True)
    var = jnp.mean(centered * centered, axis=-1, keepdims=True)
    return centered * lax.rsqrt(var + LN_EPS)


def dot(a, b):
    return jnp.dot(a, b, preferred_element_type=F32)


def iota(shape, axis):
    return lax.broadcasted_iota(jnp.int32, shape, axis)


QKV = 3 * WIDTH
WEIGHTS = 3


def pieces(l):
    third = 5 * LANES
    cols = ((0, third, 0), (third, third, 1), (2 * third, 6 * LANES, 2))
    down = [(2, l, 0, 48, 0, WIDTH, 0), (2, l, 48, 48, 0, WIDTH, 1), (2, l, 96, SLOTS, 0, WIDTH, 2)]
    qo, up = ([(m, l, 0, SLOTS, *c) for c in cols] for m in range(2))
    return [qo, up, down] if l == 0 else [qo, down, up]


PIECES = pieces(0) + pieces(1) + [[(WEIGHTS, 0, 0, HEADS, 0, LANES, 0)]]
VEC = len(PIECES) - 1
N_VEC = 10
ITEMS = [item for piece in PIECES for item in piece]
KEYS = list(dict.fromkeys(item[:2] for item in ITEMS))
FIRST = [sum(len(piece) for piece in PIECES[:p]) for p in range(len(PIECES) + 1)]


def attend(h, pos, posb, qs, kn, vn, k_in, v_in, k_out, v_out, sc, pr, ctxt):
    tiles = (HEAD // 16, 16, SEQS)
    knew = kn[h].reshape(tiles)
    vnew = vn[h].reshape(tiles)

    def insert(src, dst, s, new):
        mask = posb[...] == s.astype(BF16)
        page = jnp.where(mask[None], new, src(s).reshape(tiles)).reshape(HEAD, SEQS)
        dst(s, page)
        return page.astype(F32)

    def score(s, carry):
        page = insert(k_in, k_out, s, knew)
        sc[pl.ds(s, 1), :] = jnp.sum(page * qs[h], axis=0, keepdims=True)
        return carry

    lax.fori_loop(0, SLOTS, score, 0, unroll=8)
    sm = jnp.where(iota((SLOTS, SEQS), 0) <= pos, sc[...], -jnp.inf)
    ex = jnp.exp(sm - jnp.max(sm, axis=0, keepdims=True))
    probs = ex / jnp.sum(ex, axis=0, keepdims=True)
    pr[...] = probs.astype(BF16).astype(F32)

    def mix(s, acc):
        page = insert(v_in, v_out, s, vnew)
        return acc + page * pr[pl.ds(s, 1), :]

    ctx = lax.fori_loop(0, SLOTS, mix, jnp.zeros((HEAD, SEQS), F32), unroll=8)
    ctxt[h] = ctx.astype(BF16).astype(F32)


def attn_out(ctxt, w_ref, bias):
    ctx = ctxt[...].reshape(WIDTH, SEQS).T.astype(BF16)
    return dot(ctx, w_ref[:, :, :, :, :, QKV:].reshape(WIDTH, WIDTH)) + bias


def mlp_in(h, w_ref, bias_ref, l, act, n0, n1):
    for n in range(n0, n1):
        cols = slice(n * SEQS, (n + 1) * SEQS)
        w = w_ref[:, :, :, :, :, cols].reshape(WIDTH, SEQS)
        act[:, cols] = gelu(dot(h[...], w) + bias_ref[l, n]).astype(BF16)


def gather_kernel(x_in, pos_in, *refs):
    gather_body(x_in, pos_in, refs[:N_VEC], *refs[N_VEC:-N_VEC], refs[-N_VEC:])


def gather_body(x_in, pos_in, vec_in, wq_in, wo_in, wi_in, wd_in, kc_in, vc_in,
                  ko0, vo0, ko1, vo1, wqo1, wi1, wd1, qs, kn, vn, ctxt, hcur, h2s, lnp, bin_, pos_ref,
                  wqo0, wi0, wd0, vecs, bqkv, sc, pr, act, accr, posb,
                  local_sem, cache_sem, small_sem, send_sem, recv_sem, vec_ref):
    me = lax.axis_index('dp')
    core = me % 2
    px = (me // 2) % 2
    py = (me // 4) % 2
    pz = me // 8
    place = (px, py, pz)
    peer_core = me + 1 - 2 * core
    peers = (me + 2 - 4 * px, me + 4 - 8 * py, me + 8 - 16 * pz)

    def whole(m, l):
        if m == WEIGHTS:
            return vecs
        return ((wqo0, wi0, wd0), (wqo1, wi1, wd1))[l][m]

    def place_own(m, l):
        own = whole(m, l).at[pz, py, px, core]
        sem = local_sem.at[m, l]
        parts_in = [((wi_in, wd_in)[m - 1].at[l], own)]
        if m == 0:
            parts_in = [(wq_in.at[l], own.at[:, pl.ds(0, QKV)]), (wo_in.at[l], own.at[:, pl.ds(QKV, WIDTH)])]
        for src, dst in parts_in:
            pltpu.make_async_copy(src, dst, sem).start()

    place_own(0, 0)
    barrier = pltpu.get_barrier_semaphore()
    for peer in peers + (peer_core,):
        pl.semaphore_signal(barrier, inc=1, device_id=(peer,), device_id_type=MESH)
    small = []
    for src, dst in zip((*vec_in, pos_in, x_in), (*vec_ref, pos_ref, hcur)):
        small.append(pltpu.make_async_copy(src, dst, small_sem.at[len(small)]))
        small[-1].start()
    for l in range(LAYERS):
        for m in range(WEIGHTS):
            if m + l:
                place_own(m, l)
    for copy in small[:N_VEC]:
        copy.wait()
    g1, b1, g2, b2, bo, bd, bq, bi, gf, bf = (ref[...].astype(F32) for ref in vec_ref)
    pad = jnp.zeros((LAYERS, 32), F32)
    groups = ([g1, b1, g2, b2], [bo, bd, jnp.concatenate([gf, bf], axis=0), pad], [bq, pad])
    rows = [jnp.concatenate(group, axis=1) for group in groups] + [bi]
    vecs[pz, py, px, core] = jnp.concatenate(rows, axis=0).astype(BF16)
    pl.semaphore_wait(barrier, len(peers) + 1)

    def remote(ref, key, stage, peer):
        k = KEYS.index(key)
        stage = min(stage, 3)
        return pltpu.make_async_remote_copy(
            src_ref=ref, dst_ref=ref, send_sem=send_sem.at[k // (LAYERS * WEIGHTS), stage],
            recv_sem=recv_sem.at[k, stage], device_id=(peer,), device_id_type=MESH)

    def parts(key, stage):
        at = ([pz, py, px], [pz, py, ALL], [pz, ALL, ALL], [ALL] * 3)[stage]
        return remote(whole(*key).at[(*at, core)], key, stage, peer_core)

    def landed(p, stage):
        for key in keys(p):
            parts(key, stage).wait_recv()
            yield from (i for i in ids(p) if ITEMS[i][:2] == key)

    def send(i, stage):
        m, l, r0, rn, c0, cn, o = ITEMS[i]
        axes = [(o + s) % 3 for s in range(3)]
        at = [place[2], place[1], place[0]]
        for ax in axes[:min(stage, 2)]:
            at[2 - ax] = ALL
        if stage == 4:
            at[2 - axes[2]] = 1 - place[axes[2]]
        ref = whole(m, l).at[(*at, core, pl.ds(r0, rn), pl.ds(c0, cn))]
        peer = peers[axes[stage]] if stage < 3 else peer_core
        remote(ref, (m, l), stage, peer).start()

    def ids(p):
        return range(FIRST[p], FIRST[p + 1])

    def keys(p):
        return list(dict.fromkeys(ITEMS[i][:2] for i in ids(p)))

    def a(p):
        for key in keys(p):
            m, l = key
            if m < WEIGHTS:
                own = whole(m, l).at[pz, py, px, core]
                pltpu.make_async_copy(own, own, local_sem.at[m, l]).wait()
        for i in ids(p):
            send(i, 0)

    def b(p):
        for i in landed(p, 0):
            send(i, 1)

    def c(p):
        for i in landed(p, 1):
            send(i, 2)
            send(i, 3)

    def d(p):
        for i in landed(p, 2):
            send(i, 4)

    def e(p):
        list(landed(p, 3))

    a(0)
    a(VEC)
    a(1)
    a(2)
    cache = []
    ko, vo = (ko0, ko1), (vo0, vo1)
    for l in range(LAYERS):
        for src, dst in ((kc_in, ko), (vc_in, vo)):
            cache.append(pltpu.make_async_copy(src.at[l], dst[l], cache_sem.at[len(cache)]))
            cache[-1].start()

    for copy in small[N_VEC:]:
        copy.wait()
    pos = pos_ref[...]
    posf = pos.astype(F32)
    posb[...] = jnp.broadcast_to(posf, posb.shape).astype(BF16)
    half = (8, SEQS)
    inv_freq = jnp.full(half, 1.0, F32)
    for i in range(1, 8):
        inv_freq = jnp.where(iota(half, 0) == i, F32(ROPE_BASE ** (-i / 8.0)), inv_freq)
    angle = jnp.broadcast_to(posf, half) * inv_freq
    cos_t = jnp.cos(angle)
    sin_t = jnp.sin(angle)

    b(VEC)
    b(0)
    b(1)
    c(VEC)
    c(0)
    a(3)
    b(2)
    d(VEC)
    e(VEC)

    vall = vecs[...].reshape(16, 8, LANES).astype(F32)
    wide_shape = (16, WIDTH)
    spread = jnp.where(iota((LANES, WIDTH), 0) % 32 == iota((LANES, WIDTH), 1) % 32, 1.0, 0.0).astype(BF16)
    own = iota(wide_shape, 1) // 32 == iota(wide_shape, 0)
    quarter = iota((16, LANES), 1) // 32
    qkv_shape = (LANES, 3 * WIDTH)
    spread_q = jnp.where(iota(qkv_shape, 0) == iota(qkv_shape, 1) % 96, 1.0, 0.0).astype(BF16)
    own_q = iota((16, 3 * WIDTH), 1) // 96 == iota((16, 3 * WIDTH), 0)

    def collapse(mask, part, table):
        return jnp.sum(jnp.where(mask, dot(part.astype(BF16), table), 0.0), axis=0, keepdims=True)

    for l in range(LAYERS):
        for k in range(7):
            part = jnp.where(quarter == k % 4, vall[:, 2 * (k // 4) + l, :], 0.0)
            lnp[l, k] = collapse(own, part, spread)
        bqkv[l] = collapse(own_q, vall[:, 4 + l, :], spread_q)
        share = vall[:, 6 + l, :]
        for n in range(8):
            bin_[l, n] = jnp.concatenate([share[2 * n:2 * n + 1], share[2 * n + 1:2 * n + 2]], axis=1)

    def rope(t):
        r1, r2 = t[:8], t[8:16]
        rot = jnp.concatenate([r1 * cos_t - r2 * sin_t, r2 * cos_t + r1 * sin_t, t[16:]], axis=0)
        return rot.astype(BF16)

    def qkv_stage(l):
        normed = normalize(hcur[...].astype(F32))
        h1 = (normed * lnp[l, 0] + lnp[l, 1]).astype(BF16)
        h2s[...] = (normed * lnp[l, 2] + lnp[l, 3]).astype(BF16)
        for j in range(HEADS // 2):
            cols = slice(PAIR * j, PAIR * (j + 1))
            y = dot(h1, whole(0, l)[:, :, :, :, :, cols].reshape(WIDTH, PAIR)) + bqkv[l][:, cols]
            yt = y.astype(BF16).astype(F32).T
            for g in range(2):
                q, k, v = (yt[HEAD * (3 * g + i):HEAD * (3 * g + i + 1)] for i in range(3))
                qs[2 * j + g] = rope(q).astype(F32) * (HEAD ** -0.5)
                kn[2 * j + g] = rope(k)
                vn[2 * j + g] = v.astype(BF16)

    def heads(l, h0, h1):
        def one_head(h, carry):
            def put(ref):
                def store(s, page):
                    ref[s, h] = page
                return store
            attend(h, pos, posb, qs, kn, vn, lambda s: ko[l][s, h], lambda s: vo[l][s, h],
                   put(ko[l]), put(vo[l]), sc, pr, ctxt)
            return carry

        lax.fori_loop(h0, h1, one_head, 0)

    c(1)
    d(0)
    a(4)
    b(3)
    e(0)
    c(2)
    qkv_stage(0)
    cache[0].wait()
    cache[1].wait()
    heads(0, 0, 4)
    a(5)
    b(4)
    d(1)
    heads(0, 4, 6)
    c(3)
    heads(0, 6, HEADS)
    accr[...] = attn_out(ctxt, wqo0, lnp[0, 4])
    e(1)
    b(5)
    mlp_in(h2s, wi0, bin_, 0, act, 0, 4)
    d(2)
    mlp_in(h2s, wi0, bin_, 0, act, 4, 8)
    c(4)
    e(2)
    for j in range(2):
        cols = slice(SEQS * j, SEQS * (j + 1))
        m = dot(act[...], wd0[:, :, :, :, :, cols].reshape(FF, SEQS)) + lnp[0, 5][:, cols]
        hcur[:, cols] = (hcur[:, cols].astype(F32) + accr[:, cols] + m).astype(BF16)
    d(3)
    c(5)
    e(3)
    qkv_stage(1)
    cache[2].wait()
    cache[3].wait()
    heads(1, 0, EARLY)
    d(4)
    d(5)
    e(4)
    e(5)
    for stage in range(4):
        pages = ko0.at[pl.ds(0, WEIGHTS * 2 ** stage)]
        remote(pages, KEYS[0], stage, peer_core).wait_send()
        parts(KEYS[-1], stage).wait_send()


def finish_kernel(ko0, vo0, ko1, vo1, wqo1, wi1, wd1, qs, kn, vn, ctxt, hcur, h2s, lnp, bin_, pos_ref,
                  out_hbm, k_hbm, v_hbm, kst, vst, ctxs, sc, pr, posb, act, outs, sems):
    last = LAYERS - 1
    outputs = (k_hbm, v_hbm, out_hbm)

    def write(src, n, *at):
        dst = outputs[n].at[at] if at else outputs[n]
        pltpu.make_async_copy(src, dst, sems.at[n]).start()

    for n, src in enumerate((ko0, vo0)):
        for g in range(2):
            part = pl.ds(g * (SLOTS // 2), SLOTS // 2)
            write(src.at[part], n, 0, part)
    for n, src in enumerate((ko1, vo1)):
        write(src.at[:, pl.ds(0, EARLY)], n, last, ALL, pl.ds(0, EARLY))
    pos = pos_ref[...]
    posb[...] = jnp.broadcast_to(pos.astype(F32), posb.shape).astype(BF16)
    ctxs[...] = ctxt[...]

    def put(ref, i):
        def store(s, page):
            ref[i, s] = page
        return store

    for i in range(HEADS - EARLY):
        h = EARLY + i
        attend(h, pos, posb, qs, kn, vn, lambda s: ko1[s, h], lambda s: vo1[s, h],
               put(kst, i), put(vst, i), sc, pr, ctxs)
        write(kst.at[i], 0, last, ALL, h)
        write(vst.at[i], 1, last, ALL, h)
    mlp_in(h2s, wi1, bin_, last, act, 0, 8)
    x = attn_out(ctxs, wqo1, lnp[last, 4])
    m = dot(act[...], wd1[...].reshape(FF, WIDTH)) + lnp[last, 5]
    x = (hcur[...].astype(F32) + x + m).astype(BF16).astype(F32)
    outs[...] = (normalize(x) * lnp[0, 6] + lnp[1, 6]).astype(BF16)
    write(outs, 2)
    for n, ref in enumerate(outputs):
        pltpu.make_async_copy(ref, ref, sems.at[n]).wait()


def solution(mesh):
    row_spec = P('dp', None)
    vec_spec = P(None, 'dp')
    mat_spec = P(None, 'dp', None)
    cache_spec = P(None, 'dp', None, None, None)
    in_specs = (row_spec, P('dp'), cache_spec, cache_spec, vec_spec, vec_spec, vec_spec, vec_spec, mat_spec, vec_spec, mat_spec, vec_spec, mat_spec, vec_spec, mat_spec, vec_spec, P('dp'), P('dp'))
    out_specs = (row_spec, cache_spec, cache_spec)

    def device_step(x_embed, positions, k_cache, v_cache, ln1_gain, ln1_bias, ln2_gain, ln2_bias, w_qkv, b_qkv, w_out, b_out, w_in, b_in, w_down, b_down, lnf_gain, lnf_bias):
        vectors = (ln1_gain, ln1_bias, ln2_gain, ln2_bias, b_out, b_down, b_qkv, b_in,
                   lnf_gain.reshape(1, 32), lnf_bias.reshape(1, 32))
        to_lanes = (0, 2, 3, 4, 1)
        kt = jnp.transpose(k_cache, to_lanes)
        vt = jnp.transpose(v_cache, to_lanes)
        pos = positions.reshape(1, SEQS)
        vmem = pl.BlockSpec(memory_space=pltpu.VMEM)
        hbm = pl.BlockSpec(memory_space=pl.ANY)
        cache_shape = (LAYERS, SLOTS, HEADS, HEAD, SEQS)
        head_shape = (HEADS, HEAD, SEQS)
        in_w = GRID[1:] + (SLOTS, FF)
        down_w = GRID[1:] + (LANES, WIDTH)
        carried = [pltpu.VMEM(shape, dtype) for shape, dtype in (
            *[(cache_shape[1:], BF16)] * 4, (in_w, BF16), (in_w, BF16), (down_w, BF16),
            (head_shape, F32), (head_shape, BF16), (head_shape, BF16), (head_shape, F32),
            ((SEQS, WIDTH), BF16), ((SEQS, WIDTH), BF16), ((LAYERS, 8, 1, WIDTH), F32),
            ((LAYERS, 8, 1, SEQS), F32), ((1, SEQS), jnp.int32))]
        state = pl.pallas_call(
            gather_kernel,
            out_shape=carried,
            in_specs=[hbm] * (8 + N_VEC),
            out_specs=[vmem] * len(carried),
            scratch_shapes=[
                pltpu.VMEM(in_w, BF16),
                pltpu.VMEM(in_w, BF16),
                pltpu.VMEM(down_w, BF16),
                pltpu.VMEM(GRID[1:] + (8, LANES), BF16),
                pltpu.VMEM((LAYERS, 1, 3 * WIDTH), F32),
                pltpu.VMEM((SLOTS, SEQS), F32),
                pltpu.VMEM((SLOTS, SEQS), F32),
                pltpu.VMEM((SEQS, FF), BF16),
                pltpu.VMEM((SEQS, WIDTH), F32),
                pltpu.VMEM((16, SEQS), BF16),
                pltpu.SemaphoreType.DMA((WEIGHTS, LAYERS)),
                pltpu.SemaphoreType.DMA((4,)),
                pltpu.SemaphoreType.DMA((2 + N_VEC,)),
                pltpu.SemaphoreType.DMA((LAYERS, 4)),
                pltpu.SemaphoreType.DMA((len(KEYS), 4)),
                *[pltpu.VMEM(array.shape, BF16) for array in vectors],
            ],
            compiler_params=pltpu.CompilerParams(
                collective_id=0, has_side_effects=True, vmem_limit_bytes=SCOPED),
        )(x_embed, pos, *vectors, w_qkv, w_out, w_in, w_down, kt, vt)
        state = [pltpu.with_memory_space_constraint(array, pltpu.VMEM) for array in state]
        stage = pltpu.VMEM((HEADS - EARLY, SLOTS, HEAD, SEQS), BF16)
        out, ko, vo = pl.pallas_call(
            finish_kernel,
            out_shape=(pltpu.HBM((SEQS, WIDTH), BF16),
                       pltpu.HBM(cache_shape, BF16), pltpu.HBM(cache_shape, BF16)),
            in_specs=[vmem] * len(carried),
            out_specs=[pl.BlockSpec(memory_space=pltpu.HBM)] * 3,
            scratch_shapes=[
                stage, stage,
                pltpu.VMEM(head_shape, F32),
                pltpu.VMEM((SLOTS, SEQS), F32),
                pltpu.VMEM((SLOTS, SEQS), F32),
                pltpu.VMEM((16, SEQS), BF16),
                pltpu.VMEM((SEQS, FF), BF16),
                pltpu.VMEM((SEQS, WIDTH), BF16),
                pltpu.SemaphoreType.DMA((3,)),
            ],
            compiler_params=pltpu.CompilerParams(vmem_limit_bytes=SCOPED),
        )(*state)
        back = (0, 4, 1, 2, 3)
        return out, jnp.transpose(ko, back), jnp.transpose(vo, back)

    return jax.shard_map(device_step, mesh=mesh, in_specs=in_specs, out_specs=out_specs, check_vma=False)
```

```python
import jax
import jax.numpy as jnp
from jax import lax
from jax.experimental import pallas as pl
from jax.experimental.pallas import tpu as pltpu
from jax.sharding import PartitionSpec as P

LN_EPS = 1e-5
ROPE_BASE = 10000.0
F32 = jnp.float32
BF16 = jnp.bfloat16
MESH = pl.DeviceIdType.MESH
GRID = (2,) * 5
LAYERS, SEQS, WIDTH, SLOTS, HEADS, HEAD, LANES, FF = 2, 256, 512, 32, 8, 64, 128, 2048
PAIR = 6 * HEAD
EARLY = 2
ALL = slice(None)
SCOPED = 19 * 2 ** 20

ERF_NUM = (-2.72614225801306e-10, 2.77068142495902e-08, -2.10102402082508e-06,
           -5.69250639462346e-05, -7.34990630326855e-04, -2.95459980854025e-03,
           -1.60960333262415e-02)
ERF_DEN = (-1.45660718464996e-05, -2.13374055278905e-04, -1.68282697438203e-03,
           -7.37332916720468e-03, -1.42647390514189e-02)


def horner(coefs, t):
    acc = jnp.full_like(t, coefs[0])
    for coef in coefs[1:]:
        acc = acc * t + coef
    return acc


def gelu(v):
    z = v * (0.5 ** 0.5)
    u = jnp.clip(z, -4.0, 4.0)
    t = u * u
    erf = u * horner(ERF_NUM, t) / horner(ERF_DEN, t)
    erf = jnp.where(z >= 4.0, 1.0, jnp.where(z <= -4.0, -1.0, erf))
    return 0.5 * v * (1.0 + erf)


def normalize(v):
    centered = v - jnp.mean(v, axis=-1, keepdims=True)
    var = jnp.mean(centered * centered, axis=-1, keepdims=True)
    return centered * lax.rsqrt(var + LN_EPS)


def dot(a, b):
    return jnp.dot(a, b, preferred_element_type=F32)


def iota(shape, axis):
    return lax.broadcasted_iota(jnp.int32, shape, axis)


QKV = 3 * WIDTH
WEIGHTS = 3


def pieces(l):
    third = 5 * LANES
    cols = ((0, third, 0), (third, third, 1), (2 * third, 6 * LANES, 2))
    down = [(2, l, 0, 48, 0, WIDTH, 0), (2, l, 48, 48, 0, WIDTH, 1), (2, l, 96, SLOTS, 0, WIDTH, 2)]
    qo, up = ([(m, l, 0, SLOTS, *c) for c in cols] for m in range(2))
    return [qo, up, down] if l == 0 else [qo, down, up]


PIECES = pieces(0) + pieces(1) + [[(WEIGHTS, 0, 0, HEADS, 0, LANES, 0)]]
VEC = len(PIECES) - 1
N_VEC = 10
ITEMS = [item for piece in PIECES for item in piece]
KEYS = list(dict.fromkeys(item[:2] for item in ITEMS))
FIRST = [sum(len(piece) for piece in PIECES[:p]) for p in range(len(PIECES) + 1)]


def attend(h, pos, posb, qs, kn, vn, k_in, v_in, k_out, v_out, sc, pr, ctxt):
    tiles = (HEAD // 16, 16, SEQS)
    knew = kn[h].reshape(tiles)
    vnew = vn[h].reshape(tiles)

    def insert(src, dst, s, new):
        mask = posb[...] == s.astype(BF16)
        page = jnp.where(mask[None], new, src(s).reshape(tiles)).reshape(HEAD, SEQS)
        dst(s, page)
        return page.astype(F32)

    def score(s, carry):
        page = insert(k_in, k_out, s, knew)
        sc[pl.ds(s, 1), :] = jnp.sum(page * qs[h], axis=0, keepdims=True)
        return carry

    lax.fori_loop(0, SLOTS, score, 0, unroll=8)
    sm = jnp.where(iota((SLOTS, SEQS), 0) <= pos, sc[...], -jnp.inf)
    ex = jnp.exp(sm - jnp.max(sm, axis=0, keepdims=True))
    probs = ex / jnp.sum(ex, axis=0, keepdims=True)
    pr[...] = probs.astype(BF16).astype(F32)

    def mix(s, acc):
        page = insert(v_in, v_out, s, vnew)
        return acc + page * pr[pl.ds(s, 1), :]

    ctx = lax.fori_loop(0, SLOTS, mix, jnp.zeros((HEAD, SEQS), F32), unroll=8)
    ctxt[h] = ctx.astype(BF16).astype(F32)


def attn_out(ctxt, w_ref, bias):
    ctx = ctxt[...].reshape(WIDTH, SEQS).T.astype(BF16)
    return dot(ctx, w_ref[:, :, :, :, :, QKV:].reshape(WIDTH, WIDTH)) + bias


def mlp_in(h, w_ref, bias_ref, l, act, n0, n1):
    for n in range(n0, n1):
        cols = slice(n * SEQS, (n + 1) * SEQS)
        w = w_ref[:, :, :, :, :, cols].reshape(WIDTH, SEQS)
        act[:, cols] = gelu(dot(h[...], w) + bias_ref[l, n]).astype(BF16)


def gather_kernel(x_in, pos_in, *refs):
    gather_body(x_in, pos_in, refs[:N_VEC], *refs[N_VEC:-N_VEC], refs[-N_VEC:])


def gather_body(x_in, pos_in, vec_in, wq_in, wo_in, wi_in, wd_in, kc_in, vc_in,
                  ko0, vo0, ko1, vo1, wqo1, wi1, wd1, qs, kn, vn, ctxt, hcur, h2s, lnp, bin_, pos_ref,
                  wqo0, wi0, wd0, vecs, bqkv, sc, pr, act, accr, posb,
                  local_sem, cache_sem, small_sem, send_sem, recv_sem, vec_ref):
    me = lax.axis_index('dp')
    core = me % 2
    px = (me // 2) % 2
    py = (me // 4) % 2
    pz = me // 8
    place = (px, py, pz)
    peer_core = me + 1 - 2 * core
    peers = (me + 2 - 4 * px, me + 4 - 8 * py, me + 8 - 16 * pz)

    def whole(m, l):
        if m == WEIGHTS:
            return vecs
        return ((wqo0, wi0, wd0), (wqo1, wi1, wd1))[l][m]

    def place_own(m, l):
        own = whole(m, l).at[pz, py, px, core]
        sem = local_sem.at[m, l]
        parts_in = [((wi_in, wd_in)[m - 1].at[l], own)]
        if m == 0:
            parts_in = [(wq_in.at[l], own.at[:, pl.ds(0, QKV)]), (wo_in.at[l], own.at[:, pl.ds(QKV, WIDTH)])]
        for src, dst in parts_in:
            pltpu.make_async_copy(src, dst, sem).start()

    place_own(0, 0)
    barrier = pltpu.get_barrier_semaphore()
    for peer in peers + (peer_core,):
        pl.semaphore_signal(barrier, inc=1, device_id=(peer,), device_id_type=MESH)
    small = []
    for src, dst in zip((*vec_in, pos_in, x_in), (*vec_ref, pos_ref, hcur)):
        small.append(pltpu.make_async_copy(src, dst, small_sem.at[len(small)]))
        small[-1].start()
    for l in range(LAYERS):
        for m in range(WEIGHTS):
            if m + l:
                place_own(m, l)
    for copy in small[:N_VEC]:
        copy.wait()
    g1, b1, g2, b2, bo, bd, bq, bi, gf, bf = (ref[...].astype(F32) for ref in vec_ref)
    pad = jnp.zeros((LAYERS, 32), F32)
    groups = ([g1, b1, g2, b2], [bo, bd, jnp.concatenate([gf, bf], axis=0), pad], [bq, pad])
    rows = [jnp.concatenate(group, axis=1) for group in groups] + [bi]
    vecs[pz, py, px, core] = jnp.concatenate(rows, axis=0).astype(BF16)
    pl.semaphore_wait(barrier, len(peers) + 1)

    def remote(ref, key, stage, peer):
        k = KEYS.index(key)
        stage = min(stage, 3)
        return pltpu.make_async_remote_copy(
            src_ref=ref, dst_ref=ref, send_sem=send_sem.at[k // (LAYERS * WEIGHTS), stage],
            recv_sem=recv_sem.at[k, stage], device_id=(peer,), device_id_type=MESH)

    def parts(key, stage):
        at = ([pz, py, px], [pz, py, ALL], [pz, ALL, ALL], [ALL] * 3)[stage]
        return remote(whole(*key).at[(*at, core)], key, stage, peer_core)

    def landed(p, stage):
        for key in keys(p):
            parts(key, stage).wait_recv()
            yield from (i for i in ids(p) if ITEMS[i][:2] == key)

    def send(i, stage):
        m, l, r0, rn, c0, cn, o = ITEMS[i]
        axes = [(o + s) % 3 for s in range(3)]
        at = [place[2], place[1], place[0]]
        for ax in axes[:min(stage, 2)]:
            at[2 - ax] = ALL
        if stage == 4:
            at[2 - axes[2]] = 1 - place[axes[2]]
        ref = whole(m, l).at[(*at, core, pl.ds(r0, rn), pl.ds(c0, cn))]
        peer = peers[axes[stage]] if stage < 3 else peer_core
        remote(ref, (m, l), stage, peer).start()

    def ids(p):
        return range(FIRST[p], FIRST[p + 1])

    def keys(p):
        return list(dict.fromkeys(ITEMS[i][:2] for i in ids(p)))

    def a(p):
        for key in keys(p):
            m, l = key
            if m < WEIGHTS:
                own = whole(m, l).at[pz, py, px, core]
                pltpu.make_async_copy(own, own, local_sem.at[m, l]).wait()
        for i in ids(p):
            send(i, 0)

    def b(p):
        for i in landed(p, 0):
            send(i, 1)

    def c(p):
        for i in landed(p, 1):
            send(i, 2)
            send(i, 3)

    def d(p):
        for i in landed(p, 2):
            send(i, 4)

    def e(p):
        list(landed(p, 3))

    a(0)
    a(VEC)
    a(1)
    a(2)
    ko, vo = (ko0, ko1), (vo0, vo1)
    for l in range(LAYERS):
        for src, dst in ((kc_in, ko), (vc_in, vo)):
            pltpu.make_async_copy(src.at[l], dst[l], cache_sem.at[l]).start()

    def cache_here(l):
        pltpu.make_async_copy(kc_in, kc_in, cache_sem.at[l]).wait()

    for copy in small[N_VEC:]:
        copy.wait()
    pos = pos_ref[...]
    posf = pos.astype(F32)
    posb[...] = jnp.broadcast_to(posf, posb.shape).astype(BF16)
    half = (8, SEQS)
    inv_freq = jnp.full(half, 1.0, F32)
    for i in range(1, 8):
        inv_freq = jnp.where(iota(half, 0) == i, F32(ROPE_BASE ** (-i / 8.0)), inv_freq)
    angle = jnp.broadcast_to(posf, half) * inv_freq
    cos_t = jnp.cos(angle)
    sin_t = jnp.sin(angle)

    b(VEC)
    b(0)
    b(1)
    c(VEC)
    c(0)
    a(3)
    b(2)
    d(VEC)
    e(VEC)

    vall = vecs[...].reshape(16, 8, LANES).astype(F32)
    wide_shape = (16, WIDTH)
    spread = jnp.where(iota((LANES, WIDTH), 0) % 32 == iota((LANES, WIDTH), 1) % 32, 1.0, 0.0).astype(BF16)
    own = iota(wide_shape, 1) // 32 == iota(wide_shape, 0)
    quarter = iota((16, LANES), 1) // 32
    qkv_shape = (LANES, 3 * WIDTH)
    spread_q = jnp.where(iota(qkv_shape, 0) == iota(qkv_shape, 1) % 96, 1.0, 0.0).astype(BF16)
    own_q = iota((16, 3 * WIDTH), 1) // 96 == iota((16, 3 * WIDTH), 0)

    def collapse(mask, part, table):
        return jnp.sum(jnp.where(mask, dot(part.astype(BF16), table), 0.0), axis=0, keepdims=True)

    for l in range(LAYERS):
        for k in range(7):
            part = jnp.where(quarter == k % 4, vall[:, 2 * (k // 4) + l, :], 0.0)
            lnp[l, k] = collapse(own, part, spread)
        bqkv[l] = collapse(own_q, vall[:, 4 + l, :], spread_q)
        share = vall[:, 6 + l, :]
        for n in range(8):
            bin_[l, n] = jnp.concatenate([share[2 * n:2 * n + 1], share[2 * n + 1:2 * n + 2]], axis=1)

    def rope(t):
        r1, r2 = t[:8], t[8:16]
        rot = jnp.concatenate([r1 * cos_t - r2 * sin_t, r2 * cos_t + r1 * sin_t, t[16:]], axis=0)
        return rot.astype(BF16)

    def qkv_stage(l):
        normed = normalize(hcur[...].astype(F32))
        h1 = (normed * lnp[l, 0] + lnp[l, 1]).astype(BF16)
        h2s[...] = (normed * lnp[l, 2] + lnp[l, 3]).astype(BF16)
        for j in range(HEADS // 2):
            cols = slice(PAIR * j, PAIR * (j + 1))
            y = dot(h1, whole(0, l)[:, :, :, :, :, cols].reshape(WIDTH, PAIR)) + bqkv[l][:, cols]
            yt = y.astype(BF16).astype(F32).T
            for g in range(2):
                q, k, v = (yt[HEAD * (3 * g + i):HEAD * (3 * g + i + 1)] for i in range(3))
                qs[2 * j + g] = rope(q).astype(F32) * (HEAD ** -0.5)
                kn[2 * j + g] = rope(k)
                vn[2 * j + g] = v.astype(BF16)

    def heads(l, h0, h1):
        def one_head(h, carry):
            def put(ref):
                def store(s, page):
                    ref[s, h] = page
                return store
            attend(h, pos, posb, qs, kn, vn, lambda s: ko[l][s, h], lambda s: vo[l][s, h],
                   put(ko[l]), put(vo[l]), sc, pr, ctxt)
            return carry

        lax.fori_loop(h0, h1, one_head, 0)

    c(1)
    d(0)
    a(4)
    b(3)
    e(0)
    c(2)
    qkv_stage(0)
    cache_here(0)
    heads(0, 0, 4)
    a(5)
    b(4)
    d(1)
    heads(0, 4, 6)
    c(3)
    heads(0, 6, HEADS)
    accr[...] = attn_out(ctxt, wqo0, lnp[0, 4])
    e(1)
    b(5)
    mlp_in(h2s, wi0, bin_, 0, act, 0, 4)
    d(2)
    mlp_in(h2s, wi0, bin_, 0, act, 4, 8)
    c(4)
    e(2)
    for j in range(2):
        cols = slice(SEQS * j, SEQS * (j + 1))
        m = dot(act[...], wd0[:, :, :, :, :, cols].reshape(FF, SEQS)) + lnp[0, 5][:, cols]
        hcur[:, cols] = (hcur[:, cols].astype(F32) + accr[:, cols] + m).astype(BF16)
    d(3)
    c(5)
    e(3)
    qkv_stage(1)
    cache_here(1)
    heads(1, 0, EARLY)
    d(4)
    d(5)
    e(4)
    e(5)
    for stage in range(4):
        pages = ko0.at[pl.ds(0, WEIGHTS * 2 ** stage)]
        remote(pages, KEYS[0], stage, peer_core).wait_send()
        parts(KEYS[-1], stage).wait_send()


def finish_kernel(ko0, vo0, ko1, vo1, wqo1, wi1, wd1, qs, kn, vn, ctxt, hcur, h2s, lnp, bin_, pos_ref,
                  out_hbm, k_hbm, v_hbm, kst, vst, ctxs, sc, pr, posb, act, outs, sems):
    last = LAYERS - 1
    outputs = (k_hbm, v_hbm, out_hbm)

    def write(src, n, *at):
        dst = outputs[n].at[at] if at else outputs[n]
        pltpu.make_async_copy(src, dst, sems.at[n]).start()

    for n, src in enumerate((ko0, vo0)):
        for g in range(2):
            part = pl.ds(g * (SLOTS // 2), SLOTS // 2)
            write(src.at[part], n, 0, part)
    for n, src in enumerate((ko1, vo1)):
        write(src.at[:, pl.ds(0, EARLY)], n, last, ALL, pl.ds(0, EARLY))
    pos = pos_ref[...]
    posb[...] = jnp.broadcast_to(pos.astype(F32), posb.shape).astype(BF16)
    ctxs[...] = ctxt[...]

    def put(ref, i):
        def store(s, page):
            ref[i, s] = page
        return store

    for i in range(HEADS - EARLY):
        h = EARLY + i
        attend(h, pos, posb, qs, kn, vn, lambda s: ko1[s, h], lambda s: vo1[s, h],
               put(kst, i), put(vst, i), sc, pr, ctxs)
        write(kst.at[i], 0, last, ALL, h)
        write(vst.at[i], 1, last, ALL, h)
    mlp_in(h2s, wi1, bin_, last, act, 0, 8)
    x = attn_out(ctxs, wqo1, lnp[last, 4])
    m = dot(act[...], wd1[...].reshape(FF, WIDTH)) + lnp[last, 5]
    x = (hcur[...].astype(F32) + x + m).astype(BF16).astype(F32)
    outs[...] = (normalize(x) * lnp[0, 6] + lnp[1, 6]).astype(BF16)
    write(outs, 2)
    for n, ref in enumerate(outputs):
        pltpu.make_async_copy(ref, ref, sems.at[n]).wait()


def solution(mesh):
    row_spec = P('dp', None)
    vec_spec = P(None, 'dp')
    mat_spec = P(None, 'dp', None)
    cache_spec = P(None, 'dp', None, None, None)
    in_specs = (row_spec, P('dp'), cache_spec, cache_spec, vec_spec, vec_spec, vec_spec, vec_spec, mat_spec, vec_spec, mat_spec, vec_spec, mat_spec, vec_spec, mat_spec, vec_spec, P('dp'), P('dp'))
    out_specs = (row_spec, cache_spec, cache_spec)

    def device_step(x_embed, positions, k_cache, v_cache, ln1_gain, ln1_bias, ln2_gain, ln2_bias, w_qkv, b_qkv, w_out, b_out, w_in, b_in, w_down, b_down, lnf_gain, lnf_bias):
        vectors = (ln1_gain, ln1_bias, ln2_gain, ln2_bias, b_out, b_down, b_qkv, b_in,
                   lnf_gain.reshape(1, 32), lnf_bias.reshape(1, 32))
        to_lanes = (0, 2, 3, 4, 1)
        kt = jnp.transpose(k_cache, to_lanes)
        vt = jnp.transpose(v_cache, to_lanes)
        pos = positions.reshape(1, SEQS)
        vmem = pl.BlockSpec(memory_space=pltpu.VMEM)
        hbm = pl.BlockSpec(memory_space=pl.ANY)
        cache_shape = (LAYERS, SLOTS, HEADS, HEAD, SEQS)
        head_shape = (HEADS, HEAD, SEQS)
        in_w = GRID[1:] + (SLOTS, FF)
        down_w = GRID[1:] + (LANES, WIDTH)
        carried = [pltpu.VMEM(shape, dtype) for shape, dtype in (
            *[(cache_shape[1:], BF16)] * 4, (in_w, BF16), (in_w, BF16), (down_w, BF16),
            (head_shape, F32), (head_shape, BF16), (head_shape, BF16), (head_shape, F32),
            ((SEQS, WIDTH), BF16), ((SEQS, WIDTH), BF16), ((LAYERS, 8, 1, WIDTH), F32),
            ((LAYERS, 8, 1, SEQS), F32), ((1, SEQS), jnp.int32))]
        state = pl.pallas_call(
            gather_kernel,
            out_shape=carried,
            in_specs=[hbm] * (8 + N_VEC),
            out_specs=[vmem] * len(carried),
            scratch_shapes=[
                pltpu.VMEM(in_w, BF16),
                pltpu.VMEM(in_w, BF16),
                pltpu.VMEM(down_w, BF16),
                pltpu.VMEM(GRID[1:] + (8, LANES), BF16),
                pltpu.VMEM((LAYERS, 1, 3 * WIDTH), F32),
                pltpu.VMEM((SLOTS, SEQS), F32),
                pltpu.VMEM((SLOTS, SEQS), F32),
                pltpu.VMEM((SEQS, FF), BF16),
                pltpu.VMEM((SEQS, WIDTH), F32),
                pltpu.VMEM((16, SEQS), BF16),
                pltpu.SemaphoreType.DMA((WEIGHTS, LAYERS)),
                pltpu.SemaphoreType.DMA((LAYERS,)),
                pltpu.SemaphoreType.DMA((2 + N_VEC,)),
                pltpu.SemaphoreType.DMA((LAYERS, 4)),
                pltpu.SemaphoreType.DMA((len(KEYS), 4)),
                *[pltpu.VMEM(array.shape, BF16) for array in vectors],
            ],
            compiler_params=pltpu.CompilerParams(
                collective_id=0, has_side_effects=True, vmem_limit_bytes=SCOPED),
        )(x_embed, pos, *vectors, w_qkv, w_out, w_in, w_down, kt, vt)
        state = [pltpu.with_memory_space_constraint(array, pltpu.VMEM) for array in state]
        stage = pltpu.VMEM((HEADS - EARLY, SLOTS, HEAD, SEQS), BF16)
        out, ko, vo = pl.pallas_call(
            finish_kernel,
            out_shape=(pltpu.HBM((SEQS, WIDTH), BF16),
                       pltpu.HBM(cache_shape, BF16), pltpu.HBM(cache_shape, BF16)),
            in_specs=[vmem] * len(carried),
            out_specs=[pl.BlockSpec(memory_space=pltpu.HBM)] * 3,
            scratch_shapes=[
                stage, stage,
                pltpu.VMEM(head_shape, F32),
                pltpu.VMEM((SLOTS, SEQS), F32),
                pltpu.VMEM((SLOTS, SEQS), F32),
                pltpu.VMEM((16, SEQS), BF16),
                pltpu.VMEM((SEQS, FF), BF16),
                pltpu.VMEM((SEQS, WIDTH), BF16),
                pltpu.SemaphoreType.DMA((3,)),
            ],
            compiler_params=pltpu.CompilerParams(vmem_limit_bytes=SCOPED),
        )(*state)
        back = (0, 4, 1, 2, 3)
        return out, jnp.transpose(ko, back), jnp.transpose(vo, back)

    return jax.shard_map(device_step, mesh=mesh, in_specs=in_specs, out_specs=out_specs, check_vma=False)
```
